512 devices in a mesh: seq: 128 (over y, z, core), head: 4 (over x).
Axes of the slice: x: 4, y: 4, z: 16, core: 2. Of those that a mesh axis runs over, the one named last changes fastest.
Arguments:
- queries: float32 [768, 16384], P('head', 'seq'), may hold values from -6 to 6
- keys: float32 [768, 16384], P('head', 'seq'), may hold values from -6 to 6
- values: float32 [768, 16384], P('head', 'seq'), may hold values from -6 to 6
- counts: int32 [128], P('seq'), may hold values from 32 to 128
- out_weight: float32 [768, 768], P('head'), may hold values from -0.3125 to 0.3125
- cotangent: float32 [768, 16384], P('head', 'seq'), may hold values from -6 to 6
Outputs:
- output: float32 [768, 16384], P('head', 'seq')
- query_grad: float32 [768, 16384], P('head', 'seq')
- key_grad: float32 [768, 16384], P('head', 'seq')
- value_grad: float32 [768, 16384], P('head', 'seq')
- weight_grad: float32 [768, 768], P('head')
The draws below stay inside these ranges and needn't reach their ends.
All inputs are finite; a program needn't handle non-finite values.
Results may differ from the reference program's by a relative error of at most 0.0014.
Values sent between devices are 32-bit elements; how exact they have to be, the bound alone decides.
No kernel may reach another device: no remote copies, remote signals or barrier semaphores. Data moves between devices by JAX's collectives and lax.ppermute only.
A program may use at most 64 MiB of HBM per device.

```python
from functools import partial
import jax
import jax.numpy as jnp
from jax import lax

D = 768
HEADS = 12
HEAD = 64
TOKENS_PER_SHARD = 128
SPACING_LOCAL = 1
SPACING_CENTRAL = 4
SPACING_WIDE = 16
TOKEN_COUNT = 16384
LENGTH_LOCAL = 256
LENGTH_CENTRAL = 2048
N_SEQ = 128


def drawn_pair(key):
    base = jax.random.fold_in(key, 11)
    first, second = jax.random.split(base, 2)
    query_rows = jax.random.truncated_normal(first, -5.5, 5.5, (TOKEN_COUNT, D), jnp.float32)
    key_rows = jax.random.truncated_normal(second, -5.5, 5.5, (TOKEN_COUNT, D), jnp.float32)
    return (query_rows.T, key_rows.T)


def draw_queries(key, part):
    return drawn_pair(key)[0]


def draw_keys(key, part):
    return drawn_pair(key)[1]


def touch_ends(drawn, rng, low, largest):
    shape = drawn.shape
    spot = [jax.random.randint(jax.random.fold_in(rng, axis), (), 0, shape[axis]) for axis in range(len(shape))]
    drawn = drawn.at[tuple(spot)].set(low)
    longest = shape.index(max(shape))
    spot[longest] = (spot[longest] + 1) % shape[longest]
    return drawn.at[tuple(spot)].set(largest)


def with_spikes(entries, own_key, source, target, shards_of, factor):
    owner, partner = [(jnp.arange(entries.shape[axis_at]) // (entries.shape[axis_at] // shards_of)).reshape([-1 if axis == axis_at else 1 for axis in range(entries.ndim)]) for axis_at in (source, target)]
    chosen = jax.random.permutation(own_key, shards_of)[partner]
    strong = (owner == chosen) | (owner == (partner + shards_of // 2) % shards_of)
    return jnp.where(strong, factor * entries, entries)


def steps_of(key, extent, cuts, low, top_value):
    factor_of = 1.0
    for axis_at, parts in cuts:
        steps = jax.random.uniform(jax.random.fold_in(jax.random.fold_in(key, 6), axis_at), (parts,), jnp.float32, low / len(cuts), top_value / len(cuts))
        factor_of = factor_of * jnp.repeat(jnp.exp(steps), extent[axis_at] // parts).reshape((-1,) + (1,) * (len(extent) - 1 - axis_at))
    return factor_of


def normal_values(own_key, dims, spread, reach, cuts=(), kind=jnp.bfloat16):
    entries = spread * jax.random.normal(own_key, dims, jnp.float32)
    if cuts:
        entries = entries * steps_of(own_key, dims, cuts, -0.22, 0.18)
    return jnp.clip(entries, -reach, reach).astype(kind)


def bell_draw_with(stream_key, shape, width, bound, shards, heavy, held_as=jnp.bfloat16):
    values = width * jax.random.normal(stream_key, shape, jnp.float32)
    if shards:
        values = values * steps_of(stream_key, shape, shards, -0.22, 0.18)
    return jnp.clip(with_spikes(values, jax.random.fold_in(stream_key, 3), *heavy), -bound, bound).astype(held_as)


def setup_inputs(seed: int = 0) -> dict:
    arg_keys = jax.random.split(jax.random.key(seed), 7)
    return {
        "queries": draw_queries(jax.random.fold_in(arg_keys[6], 71), 0),
        "keys": draw_keys(jax.random.fold_in(arg_keys[6], 71), 0),
        "values": normal_values(arg_keys[2], (D, TOKEN_COUNT), 1.0, 6.0, ((0, 4), (1, 128)), jnp.float32),
        "counts": touch_ends(jax.random.randint(arg_keys[3], (N_SEQ,), max(TOKENS_PER_SHARD // 4, SPACING_WIDE), TOKENS_PER_SHARD + 1), jax.random.fold_in(arg_keys[3], 1), max(TOKENS_PER_SHARD // 4, SPACING_WIDE), TOKENS_PER_SHARD).astype(jnp.int32),
        "out_weight": bell_draw_with(arg_keys[4], (D, D), D ** -0.5, 0.3125, ((0, 4),), (0, 1, 4, 2.0), jnp.float32),
        "cotangent": normal_values(arg_keys[5], (D, TOKEN_COUNT), 1.0, 6.0, ((0, 4), (1, 128)), jnp.float32),
    }


PRECISE = lax.Precision.HIGHEST
MASKED_SCORE = -1e+30

def single_branch(query_per_head, key_per_head, value_per_head, active_rows, current_head, segment_span, spacing_factor):
    length, head_size = query_per_head.shape
    seg_count = length // segment_span
    per_segment = segment_span // spacing_factor
    offset = current_head % spacing_factor

    def select_rows(block):
        shaped = block.reshape((seg_count, per_segment, spacing_factor) + block.shape[1:])
        return lax.dynamic_index_in_dim(shaped, offset, 2, keepdims=False)
    q_sel = select_rows(query_per_head)
    k_sel = select_rows(key_per_head)
    v_sel = select_rows(value_per_head)
    live_sel = select_rows(active_rows)
    scores = jnp.einsum('sqe,ske->sqk', q_sel, k_sel, precision=PRECISE) * head_size ** (-0.5)
    scores = jnp.where(live_sel[:, None, :] > 0.5, scores, MASKED_SCORE)
    row_max = lax.optimization_barrier(jnp.max(scores, axis=-1))
    weights = jnp.exp(scores - row_max[..., None])
    denominator = lax.optimization_barrier(jnp.sum(weights, axis=-1))
    branch_out = jnp.einsum('sqk,ske->sqe', weights, v_sel, precision=PRECISE) / denominator[..., None]
    log_total = row_max + jnp.log(denominator)
    chosen = jnp.arange(spacing_factor, dtype=jnp.int32) == offset
    spread_out = jnp.where(chosen[None, None, :, None], branch_out[:, :, None, :], 0.0).reshape(length, head_size)
    spread_lse = jnp.where(chosen[None, None, :], log_total[:, :, None], MASKED_SCORE).reshape(length)
    return (spread_out, spread_lse)

def one_head(inputs, active_rows):
    query_per_head, key_per_head, value_per_head, current_head = inputs
    branch_pieces = [single_branch(query_per_head, key_per_head, value_per_head, active_rows, current_head, segment_span, spacing_factor) for segment_span, spacing_factor in ((LENGTH_LOCAL, SPACING_LOCAL), (LENGTH_CENTRAL, SPACING_CENTRAL), (TOKEN_COUNT, SPACING_WIDE))]
    stacked = jnp.stack([item[1] for item in branch_pieces])
    row_peak = lax.optimization_barrier(jnp.max(stacked, axis=0))
    combined_lse = row_peak + jnp.log(lax.optimization_barrier(jnp.sum(jnp.exp(stacked - row_peak[None]), axis=0)))
    combined = jnp.zeros_like(query_per_head)
    for spread_out, spread_lse in branch_pieces:
        combined = combined + jnp.exp(spread_lse - combined_lse)[:, None] * spread_out
    return combined * active_rows[:, None]

def reference(queries, keys, values, counts, out_weight, cotangent):
    positions = jnp.arange(TOKEN_COUNT, dtype=jnp.int32)
    active_rows = (positions % TOKENS_PER_SHARD < jnp.repeat(counts, TOKENS_PER_SHARD)).astype(queries.dtype)
    head_ids = jnp.arange(HEADS, dtype=jnp.int32)

    def by_heads(block):
        return block.reshape(TOKEN_COUNT, HEADS, HEAD).transpose(1, 0, 2)

    def forward(q_all, k_all, v_all, weight):
        head_step = jax.checkpoint(partial(one_head, active_rows=active_rows))
        heads_out = lax.map(head_step, (by_heads(q_all), by_heads(k_all), by_heads(v_all), head_ids))
        attended = heads_out.transpose(1, 0, 2).reshape(TOKEN_COUNT, D)
        return jnp.dot(attended, weight, precision=PRECISE, preferred_element_type=jnp.float32)
    output, pullback = jax.vjp(forward, queries.T, keys.T, values.T, out_weight)
    grads = pullback(cotangent.T)
    return (output.T, grads[0].T, grads[1].T, grads[2].T, grads[3])
```

```python
import jax
import jax.numpy as jnp
from jax import lax
from jax.experimental import pallas as pl
from jax.experimental.pallas import tpu as pltpu
from jax.sharding import Mesh
from jax.sharding import PartitionSpec as P

HEAD = 64
LOCAL_HEADS = 3
TOKENS = 128
SPACING_CENTRAL = 4
SPACING_WIDE = 16
MID_ROWS = TOKENS // SPACING_CENTRAL
FAR_ROWS = TOKENS // SPACING_WIDE
FAR_BLOCK = LOCAL_HEADS * FAR_ROWS
MID_BLOCK = LOCAL_HEADS * MID_ROWS
NEAR_BLOCK = LOCAL_HEADS * TOKENS
SCALE = HEAD ** (-0.5)
MASKED_SCORE = -1e30
DEAD_MARK = 1e6
DEAD_LEVEL = 1e5
INTERPRET = False
SEQ = ("y", "zh", "zl", "c")
Z = ("zh", "zl")


def dot(a, b, ca, cb):
    return lax.dot_general(
        a,
        b,
        (((ca,), (cb,)), ((), ())),
        precision=lax.Precision.HIGHEST,
        preferred_element_type=jnp.float32,
    )


def iota(shape, dim):
    return lax.broadcasted_iota(jnp.int32, shape, dim)


def chooser(rows, spacing, offset):
    shape = (rows, TOKENS)
    return (iota(shape, 1) == iota(shape, 0) * spacing + offset).astype(jnp.float32)


def placer(rows, spacing, offset):
    shape = (TOKENS, rows)
    return (iota(shape, 0) == iota(shape, 1) * spacing + offset).astype(jnp.float32)


def kernel_call(body, out_shape, operands, scalars):
    in_specs = [pl.BlockSpec(memory_space=pltpu.SMEM)] * scalars + [
        pl.BlockSpec(memory_space=pltpu.VMEM)
    ] * (len(operands) - scalars)
    return pl.pallas_call(
        body,
        out_shape=out_shape,
        in_specs=in_specs,
        out_specs=jax.tree.map(lambda _: pl.BlockSpec(memory_space=pltpu.VMEM), out_shape),
        interpret=INTERPRET,
    )(*operands)


def shaped(*dims):
    return jax.ShapeDtypeStruct(dims, jnp.float32)


def pack_body(count, base, k_ref, v_ref, far_ref, mid_ref, near_ref):
    feature = iota((2 * HEAD, TOKENS), 0)
    live = iota((2 * HEAD, TOKENS), 1) < count[0]
    for j in range(LOCAL_HEADS):
        rows = slice(HEAD * j, HEAD * (j + 1))
        both = jnp.concatenate([k_ref[rows, :], v_ref[rows, :]], axis=0)
        both = jnp.where(live, both, jnp.where(feature == 0, DEAD_MARK, 0.0))
        turned = both.T
        near_ref[TOKENS * j : TOKENS * (j + 1), :] = turned
        head = base[0] + j
        far = dot(chooser(FAR_ROWS, SPACING_WIDE, head % SPACING_WIDE), turned, 1, 0)
        mid = dot(chooser(MID_ROWS, SPACING_CENTRAL, head % SPACING_CENTRAL), turned, 1, 0)
        for i in range(far_ref.shape[0]):
            far_ref[i, FAR_ROWS * j : FAR_ROWS * (j + 1), :] = far
        for i in range(mid_ref.shape[0]):
            mid_ref[i, MID_ROWS * j : MID_ROWS * (j + 1), :] = mid


def query_body(count, base, q_ref, w_ref, cot_ref, far_ref, mid_ref, near_ref):
    live = iota((HEAD, TOKENS), 1) < count[0]
    grads = dot(w_ref[...], cot_ref[...], 1, 0)
    for j in range(LOCAL_HEADS):
        rows = slice(HEAD * j, HEAD * (j + 1))
        both = jnp.concatenate(
            [q_ref[rows, :] * SCALE, jnp.where(live, grads[rows, :], 0.0)], axis=0
        )
        turned = both.T
        head = base[0] + j
        near_ref[j] = turned
        far_ref[j] = dot(chooser(FAR_ROWS, SPACING_WIDE, head % SPACING_WIDE), turned, 1, 0)
        mid_ref[j] = dot(
            chooser(MID_ROWS, SPACING_CENTRAL, head % SPACING_CENTRAL), turned, 1, 0
        )


def branch_scores(turned, pairs):
    rows = turned.shape[0]
    left = iota((rows, 2 * HEAD), 1) < HEAD
    mark = ((iota((8, 2 * HEAD), 0) == 0) & (iota((8, 2 * HEAD), 1) == 0)).astype(jnp.float32)
    queries = jnp.concatenate(
        [jnp.where(left, turned, 0.0), jnp.where(left, 0.0, turned)], axis=0
    )
    products = dot(jnp.concatenate([queries, mark], axis=0), pairs, 1, 1)
    dead = products[2 * rows : 2 * rows + 1, :] > DEAD_LEVEL
    scores = jnp.where(dead, MASKED_SCORE, products[:rows])
    prob_grads = products[rows : 2 * rows]
    top = jnp.max(scores, axis=1, keepdims=True)
    weights = jnp.exp(scores - top)
    total = jnp.sum(weights, axis=1, keepdims=True)
    pulled = jnp.sum(weights * prob_grads, axis=1, keepdims=True)
    return queries, weights, prob_grads, top, total, pulled


def branch_grads(queries, weights, prob_grads, factor, delta, pairs):
    rows = weights.shape[0]
    probs = weights * factor
    score_grads = probs * (prob_grads - delta)
    both = jnp.concatenate([score_grads, probs], axis=0)
    sums = dot(both, pairs, 1, 0)
    left = iota((rows, 2 * HEAD), 1) < HEAD
    query_side = jnp.where(left, sums[:rows], sums[rows:])
    key_side = dot(both, queries, 0, 0)
    return query_side, key_side


def attention_body(
    count,
    base,
    core,
    qf_ref,
    qm_ref,
    qn_ref,
    near_own,
    near_other,
    mid_own,
    mid_other,
    far_own,
    far_other,
    w_ref,
    cot_ref,
    dq_ref,
    terms_ref,
    keep_ref,
    send_ref,
    *,
    unit_rows,
):
    units = far_own.shape[0]
    mid_units = mid_own.shape[0]
    mid_at = units * unit_rows
    near_at = mid_at + mid_units * MID_BLOCK
    lanes = iota((TOKENS, 128), 1)
    position = iota((TOKENS, 1), 0)
    attended = []
    for j in range(LOCAL_HEADS):
        head = base[0] + j
        fs = slice(FAR_ROWS * j, FAR_ROWS * (j + 1))
        ms = slice(MID_ROWS * j, MID_ROWS * (j + 1))
        ns = slice(TOKENS * j, TOKENS * (j + 1))
        far_pairs = jnp.concatenate(
            [
                far_own[:, fs, :].reshape(units * FAR_ROWS, 128),
                far_other[:, fs, :].reshape(units * FAR_ROWS, 128),
            ],
            axis=0,
        )
        mid_pairs = jnp.concatenate(
            [
                mid_own[:, ms, :].reshape(mid_units * MID_ROWS, 128),
                mid_other[:, ms, :].reshape(mid_units * MID_ROWS, 128),
            ],
            axis=0,
        )
        near_pairs = jnp.concatenate([near_own[ns, :], near_other[ns, :]], axis=0)
        far_off = head % SPACING_WIDE
        mid_off = head % SPACING_CENTRAL
        far = branch_scores(qf_ref[j], far_pairs)
        mid = branch_scores(qm_ref[j], mid_pairs)
        near = branch_scores(qn_ref[j], near_pairs)

        def columns(branch, rows):
            at = iota((rows, 128), 1)
            return jnp.where(at == 0, branch[3], jnp.where(at == 1, branch[4], branch[5]))

        far_put = placer(FAR_ROWS, SPACING_WIDE, far_off)
        mid_put = placer(MID_ROWS, SPACING_CENTRAL, mid_off)
        far_stats = dot(far_put, columns(far, FAR_ROWS), 1, 0)
        mid_stats = dot(mid_put, columns(mid, MID_ROWS), 1, 0)
        in_far = position % SPACING_WIDE == far_off
        in_mid = position % SPACING_CENTRAL == mid_off
        far_top = jnp.where(in_far, far_stats[:, 0:1], MASKED_SCORE)
        mid_top = jnp.where(in_mid, mid_stats[:, 0:1], MASKED_SCORE)
        near_top = near[3]
        top = jnp.maximum(near_top, jnp.maximum(mid_top, far_top))
        far_factor = jnp.exp(far_top - top)
        mid_factor = jnp.exp(mid_top - top)
        near_factor = jnp.exp(near_top - top)
        total = (
            near_factor * near[4]
            + mid_factor * mid_stats[:, 1:2]
            + far_factor * far_stats[:, 1:2]
        )
        far_factor = far_factor / total
        mid_factor = mid_factor / total
        near_factor = near_factor / total
        delta = (
            near_factor * near[5]
            + mid_factor * mid_stats[:, 2:3]
            + far_factor * far_stats[:, 2:3]
        )
        back = jnp.where(
            lanes == 0, far_factor, jnp.where(lanes == 1, mid_factor, delta)
        )
        far_back = dot(chooser(FAR_ROWS, SPACING_WIDE, far_off), back, 1, 0)
        mid_back = dot(chooser(MID_ROWS, SPACING_CENTRAL, mid_off), back, 1, 0)
        near_q, near_k = branch_grads(*near[:3], near_factor, delta, near_pairs)
        mid_q, mid_k = branch_grads(*mid[:3], mid_back[:, 1:2], mid_back[:, 2:3], mid_pairs)
        far_q, far_k = branch_grads(*far[:3], far_back[:, 0:1], far_back[:, 2:3], far_pairs)
        query_side = near_q + dot(mid_put, mid_q, 1, 0) + dot(far_put, far_q, 1, 0)
        turned = query_side.T
        dq_ref[HEAD * j : HEAD * (j + 1), :] = turned[:HEAD] * SCALE
        attended.append(turned[HEAD:])
        for ref, half in ((keep_ref, 0), (send_ref, 1)):
            for i in range(units):
                at = (half * units + i) * FAR_ROWS
                to = i * unit_rows + FAR_ROWS * j
                ref[to : to + FAR_ROWS, :] = far_k[at : at + FAR_ROWS]
            for i in range(mid_units):
                at = (half * mid_units + i) * MID_ROWS
                to = mid_at + i * MID_BLOCK + MID_ROWS * j
                ref[to : to + MID_ROWS, :] = mid_k[at : at + MID_ROWS]
            to = near_at + TOKENS * j
            ref[to : to + TOKENS, :] = near_k[half * TOKENS : (half + 1) * TOKENS]
    live = iota((HEAD * LOCAL_HEADS, TOKENS), 1) < count[0]
    rows = jnp.where(live, jnp.concatenate(attended, axis=0), 0.0)
    terms_ref[...] = dot(w_ref[...], rows, 0, 0)
    weight = dot(rows, cot_ref[...], 1, 1)
    wide = weight.shape[1] // 128
    tiles = [
        weight[8 * (t // wide) : 8 * (t // wide) + 8, 128 * (t % wide) : 128 * (t % wide) + 128]
        for t in range(wide * weight.shape[0] // 8)
    ]
    empty = jnp.zeros((8, 128), jnp.float32)
    first = core[0] == 0

    def tile(half, i, slot):
        t = slot * 2 * units + half * units + i
        return tiles[t] if t < len(tiles) else empty

    for i in range(units):
        for slot in range((unit_rows - FAR_BLOCK) // 8):
            low, high = tile(0, i, slot), tile(1, i, slot)
            to = i * unit_rows + FAR_BLOCK + 8 * slot
            keep_ref[to : to + 8, :] = jnp.where(first, low, high)
            send_ref[to : to + 8, :] = jnp.where(first, high, low)


def finish_body(base, far_ref, mid_ref, near_ref, other_ref, dk_ref, dv_ref):
    far_sum = far_ref[0, :FAR_BLOCK, :]
    for i in range(1, far_ref.shape[0]):
        far_sum = far_sum + far_ref[i, :FAR_BLOCK, :]
    mid_sum = mid_ref[0]
    for i in range(1, mid_ref.shape[0]):
        mid_sum = mid_sum + mid_ref[i]
    for j in range(LOCAL_HEADS):
        head = base[0] + j
        ns = slice(TOKENS * j, TOKENS * (j + 1))
        far_put = placer(FAR_ROWS, SPACING_WIDE, head % SPACING_WIDE)
        mid_put = placer(MID_ROWS, SPACING_CENTRAL, head % SPACING_CENTRAL)
        both = (
            near_ref[ns, :]
            + other_ref[ns, :]
            + dot(mid_put, mid_sum[MID_ROWS * j : MID_ROWS * (j + 1)], 1, 0)
            + dot(far_put, far_sum[FAR_ROWS * j : FAR_ROWS * (j + 1)], 1, 0)
        )
        turned = both.T
        dk_ref[HEAD * j : HEAD * (j + 1), :] = turned[:HEAD]
        dv_ref[HEAD * j : HEAD * (j + 1), :] = turned[HEAD:]


def exchange(pieces, axis):
    dims = pieces.shape
    flat = pieces.reshape(dims[0] * dims[1], dims[2])
    return lax.all_to_all(flat, axis, 0, 0, tiled=True).reshape(dims)


def from_partner(x):
    return lax.ppermute(x, "c", [(0, 1), (1, 0)])


def on_device(queries, keys, values, counts, out_weight, cotangent):
    ny, nz, nzl = lax.axis_size("y"), lax.axis_size(Z), lax.axis_size("zl")
    heads = lax.axis_size("h")
    columns, tokens = queries.shape
    base = (lax.axis_index("h") * LOCAL_HEADS).astype(jnp.int32).reshape(1)
    core = lax.axis_index("c").astype(jnp.int32).reshape(1)

    cot = exchange(jnp.broadcast_to(cotangent, (heads, columns, tokens)), "h")
    full_cot = cot.reshape(heads * columns, tokens)

    far_out, mid_out, near_own = kernel_call(
        pack_body,
        (shaped(nz, FAR_BLOCK, 128), shaped(nzl, MID_BLOCK, 128), shaped(NEAR_BLOCK, 128)),
        (counts, base, keys, values),
        2,
    )
    near_other = from_partner(near_own)
    far_line = exchange(far_out, Z)
    mid_own = exchange(mid_out, "zl")
    mid_other = from_partner(mid_own)
    far_plane = exchange(
        jnp.broadcast_to(far_line.reshape(1, nz * FAR_BLOCK, 128), (ny, nz * FAR_BLOCK, 128)), "y"
    )
    far_own = far_plane.reshape(ny * nz, FAR_BLOCK, 128)
    far_other = from_partner(far_own)

    query_far, query_mid, query_near = kernel_call(
        query_body,
        (
            shaped(LOCAL_HEADS, FAR_ROWS, 128),
            shaped(LOCAL_HEADS, MID_ROWS, 128),
            shaped(LOCAL_HEADS, TOKENS, 128),
        ),
        (counts, base, queries, out_weight, full_cot),
        2,
    )
    units = ny * nz
    tiles = out_weight.size // 1024
    slots = -(-tiles // (2 * units))
    unit_rows = FAR_BLOCK + 8 * slots
    rows = units * unit_rows + nzl * MID_BLOCK + NEAR_BLOCK
    query_grad, terms, keep, send = kernel_call(
        lambda *refs: attention_body(*refs, unit_rows=unit_rows),
        (shaped(columns, tokens), shaped(heads * columns, tokens), shaped(rows, 128), shaped(rows, 128)),
        (
            counts,
            base,
            core,
            query_far,
            query_mid,
            query_near,
            near_own,
            near_other,
            mid_own,
            mid_other,
            far_own,
            far_other,
            out_weight,
            full_cot,
        ),
        3,
    )
    received = from_partner(send)
    output = jnp.sum(exchange(terms.reshape(heads, columns, tokens), "h"), axis=0)

    mid_at = units * unit_rows
    near_at = mid_at + nzl * MID_BLOCK
    plane = (keep[:mid_at] + received[:mid_at]).reshape(ny, nz * unit_rows, 128)
    line = jnp.sum(exchange(plane, "y"), axis=0).reshape(nz, unit_rows, 128)
    parts = exchange(line, Z)
    mid_sums = exchange(
        (keep[mid_at:near_at] + received[mid_at:near_at]).reshape(nzl, MID_BLOCK, 128), "zl"
    )
    key_grad, value_grad = kernel_call(
        finish_body,
        (shaped(columns, tokens), shaped(columns, tokens)),
        (base, parts, mid_sums, keep[near_at:], received[near_at:]),
        1,
    )

    own_tiles = jnp.sum(parts[:, FAR_BLOCK:], axis=0)
    depth = 8 * slots
    in_line = exchange(jnp.broadcast_to(own_tiles, (nz, depth, 128)), Z)
    in_plane = exchange(
        jnp.broadcast_to(in_line.reshape(1, nz * depth, 128), (ny, nz * depth, 128)), "y"
    )
    own_half = in_plane.reshape(units, depth, 128)
    other_half = from_partner(own_half)
    first = core[0] == 0
    everything = jnp.stack(
        [jnp.where(first, own_half, other_half), jnp.where(first, other_half, own_half)]
    ).reshape(2 * units, slots, 8, 128)
    ordered = everything.swapaxes(0, 1).reshape(2 * units * slots, 8, 128)[:tiles]
    wide = out_weight.shape[1] // 128
    weight_grad = (
        ordered.reshape(tiles // wide, wide, 8, 128).swapaxes(1, 2).reshape(out_weight.shape)
    )
    return output, query_grad, key_grad, value_grad, weight_grad


def solution(mesh):
    split = Mesh(
        mesh.devices.reshape(4, 2, 8, 2, mesh.shape["head"]), ("y", "zh", "zl", "c", "h")
    )
    return on_mesh(split)


def on_mesh(split):
    in_specs = (
        P("h", SEQ),
        P("h", SEQ),
        P("h", SEQ),
        P(SEQ),
        P("h", None),
        P("h", SEQ),
    )
    out_specs = (P("h", SEQ), P("h", SEQ), P("h", SEQ), P("h", SEQ), P("h", None))
    return jax.shard_map(
        on_device, mesh=split, in_specs=in_specs, out_specs=out_specs, check_vma=False
    )
```

```python
import jax
import jax.numpy as jnp
from jax import lax
from jax.experimental import pallas as pl
from jax.experimental.pallas import tpu as pltpu
from jax.sharding import Mesh
from jax.sharding import PartitionSpec as P

HEAD = 64
LOCAL_HEADS = 3
TOKENS = 128
SPACING_CENTRAL = 4
SPACING_WIDE = 16
MID_ROWS = TOKENS // SPACING_CENTRAL
FAR_ROWS = TOKENS // SPACING_WIDE
FAR_BLOCK = LOCAL_HEADS * FAR_ROWS
MID_BLOCK = LOCAL_HEADS * MID_ROWS
NEAR_BLOCK = LOCAL_HEADS * TOKENS
SCALE = HEAD ** (-0.5)
MASKED_SCORE = -1e30
DEAD_MARK = 1e6
DEAD_LEVEL = 1e5
INTERPRET = False
SEQ = ("y", "zh", "zl", "c")
Z = ("zh", "zl")


def dot(a, b, ca, cb):
    return lax.dot_general(
        a,
        b,
        (((ca,), (cb,)), ((), ())),
        precision=lax.Precision.HIGHEST,
        preferred_element_type=jnp.float32,
    )


def halves(x):
    high = x.astype(jnp.bfloat16)
    return high, (x - high.astype(jnp.float32)).astype(jnp.bfloat16)


def dot3(a, b, ca, cb):
    a_high, a_low = halves(a)
    b_high, b_low = halves(b)

    def one(x, y):
        return lax.dot_general(
            x, y, (((ca,), (cb,)), ((), ())), preferred_element_type=jnp.float32
        )

    return one(a_low, b_high) + one(a_high, b_low) + one(a_high, b_high)


def iota(shape, dim):
    return lax.broadcasted_iota(jnp.int32, shape, dim)


def chooser(rows, spacing, offset):
    shape = (rows, TOKENS)
    return (iota(shape, 1) == iota(shape, 0) * spacing + offset).astype(jnp.float32)


def placer(rows, spacing, offset):
    shape = (TOKENS, rows)
    return (iota(shape, 0) == iota(shape, 1) * spacing + offset).astype(jnp.float32)


def kernel_call(body, out_shape, operands, scalars):
    in_specs = [pl.BlockSpec(memory_space=pltpu.SMEM)] * scalars + [
        pl.BlockSpec(memory_space=pltpu.VMEM)
    ] * (len(operands) - scalars)
    return pl.pallas_call(
        body,
        out_shape=out_shape,
        in_specs=in_specs,
        out_specs=jax.tree.map(lambda _: pl.BlockSpec(memory_space=pltpu.VMEM), out_shape),
        interpret=INTERPRET,
    )(*operands)


def shaped(*dims):
    return jax.ShapeDtypeStruct(dims, jnp.float32)


def pack_body(count, base, k_ref, v_ref, far_ref, mid_ref, near_ref):
    feature = iota((2 * HEAD, TOKENS), 0)
    live = iota((2 * HEAD, TOKENS), 1) < count[0]
    for j in range(LOCAL_HEADS):
        rows = slice(HEAD * j, HEAD * (j + 1))
        both = jnp.concatenate([k_ref[rows, :], v_ref[rows, :]], axis=0)
        both = jnp.where(live, both, jnp.where(feature == 0, DEAD_MARK, 0.0))
        turned = both.T
        near_ref[TOKENS * j : TOKENS * (j + 1), :] = turned
        head = base[0] + j
        far = dot(chooser(FAR_ROWS, SPACING_WIDE, head % SPACING_WIDE), turned, 1, 0)
        mid = dot(chooser(MID_ROWS, SPACING_CENTRAL, head % SPACING_CENTRAL), turned, 1, 0)
        for i in range(far_ref.shape[0]):
            far_ref[i, FAR_ROWS * j : FAR_ROWS * (j + 1), :] = far
        for i in range(mid_ref.shape[0]):
            mid_ref[i, MID_ROWS * j : MID_ROWS * (j + 1), :] = mid


def query_body(count, base, q_ref, w_ref, own_ref, one_ref, two_ref, three_ref, *outs):
    far_ref, mid_ref, near_ref, cot_ref = outs
    columns = own_ref.shape[0]
    heads = cot_ref.shape[0] // columns
    group = base[0] // LOCAL_HEADS
    for k, ref in enumerate((own_ref, one_ref, two_ref, three_ref)):
        at = pl.multiple_of(columns * ((group + heads - k) % heads), columns)
        cot_ref[pl.ds(at, columns), :] = ref[...]
    live = iota((HEAD, TOKENS), 1) < count[0]
    grads = dot(w_ref[...], cot_ref[...], 1, 0)
    for j in range(LOCAL_HEADS):
        rows = slice(HEAD * j, HEAD * (j + 1))
        both = jnp.concatenate(
            [q_ref[rows, :] * SCALE, jnp.where(live, grads[rows, :], 0.0)], axis=0
        )
        turned = both.T
        head = base[0] + j
        near_ref[j] = turned
        far_ref[j] = dot(chooser(FAR_ROWS, SPACING_WIDE, head % SPACING_WIDE), turned, 1, 0)
        mid_ref[j] = dot(
            chooser(MID_ROWS, SPACING_CENTRAL, head % SPACING_CENTRAL), turned, 1, 0
        )


def split_queries(turned):
    left = iota(turned.shape, 1) < HEAD
    return jnp.concatenate([jnp.where(left, turned, 0.0), jnp.where(left, 0.0, turned)], axis=0)


def branch_scores(turned, pairs):
    rows = turned.shape[0]
    mark = ((iota((8, 2 * HEAD), 0) == 0) & (iota((8, 2 * HEAD), 1) == 0)).astype(jnp.float32)
    products = dot(jnp.concatenate([split_queries(turned), mark], axis=0), pairs, 1, 1)
    dead = products[2 * rows : 2 * rows + 1, :] > DEAD_LEVEL
    scores = jnp.where(dead, MASKED_SCORE, products[:rows])
    prob_grads = products[rows : 2 * rows]
    top = jnp.max(scores, axis=1, keepdims=True)
    weights = jnp.exp(scores - top)
    total = jnp.sum(weights, axis=1, keepdims=True)
    pulled = jnp.sum(weights * prob_grads, axis=1, keepdims=True)
    at = iota((rows, 128), 1)
    stats = jnp.where(at == 0, top, jnp.where(at == 1, total, pulled))
    return jnp.concatenate([prob_grads, weights], axis=0), stats


def branch_grads(both, factor, delta):
    rows = both.shape[0] // 2
    probs = both[rows:] * factor
    return jnp.concatenate([probs * (both[:rows] - delta), probs], axis=0)


def query_side(both, pairs):
    rows = both.shape[0] // 2
    sums = dot3(both, pairs, 1, 0)
    left = iota((rows, 2 * HEAD), 1) < HEAD
    return jnp.where(left, sums[:rows], sums[rows:])


def gathered(refs, rows):
    parts = []
    for ref in refs:
        part = ref[:, rows, :]
        parts.append(part.reshape(part.shape[0] * part.shape[1], 128))
    return jnp.concatenate(parts, axis=0)


def head_slice(j, rows):
    return slice(rows * j, rows * (j + 1))


def near_pairs_of(own, other, j):
    rows = head_slice(j, TOKENS)
    return jnp.concatenate([own[rows, :], other[rows, :]], axis=0)


def scores_body(*refs):
    qf_ref, qn_ref, near_own, near_other = refs[:4]
    far_refs = refs[4:-4]
    far_both, far_stats, near_both, near_stats = refs[-4:]
    for j in range(LOCAL_HEADS):
        pairs = gathered(far_refs, head_slice(j, FAR_ROWS))
        far_both[j], far_stats[j] = branch_scores(qf_ref[j], pairs)
        near_both[j], near_stats[j] = branch_scores(
            qn_ref[j], near_pairs_of(near_own, near_other, j)
        )


def attention_body(*refs):
    count, base = refs[:2]
    qm_ref, near_own, near_other, mid_own, mid_other, w_ref, cot_ref = refs[2:9]
    far_in, far_stats_ref, near_in, near_stats_ref = refs[9:13]
    outs = refs[-10:]
    far_refs = refs[13:-10]
    dq_ref, weight_ref, far_both, mid_both, near_both = outs[:5]
    term_refs, terms_ref = outs[5:9], outs[9]
    lanes = iota((TOKENS, 128), 1)
    position = iota((TOKENS, 1), 0)
    attended = []
    for j in range(LOCAL_HEADS):
        head = base[0] + j
        far_off = head % SPACING_WIDE
        mid_off = head % SPACING_CENTRAL
        mid_pairs = gathered((mid_own, mid_other), head_slice(j, MID_ROWS))
        mid_start, mid_column = branch_scores(qm_ref[j], mid_pairs)
        far_put = placer(FAR_ROWS, SPACING_WIDE, far_off)
        mid_put = placer(MID_ROWS, SPACING_CENTRAL, mid_off)
        far_stats = dot(far_put, far_stats_ref[j], 1, 0)
        mid_stats = dot(mid_put, mid_column, 1, 0)
        near_stats = near_stats_ref[j]
        in_far = position % SPACING_WIDE == far_off
        in_mid = position % SPACING_CENTRAL == mid_off
        far_top = jnp.where(in_far, far_stats[:, 0:1], MASKED_SCORE)
        mid_top = jnp.where(in_mid, mid_stats[:, 0:1], MASKED_SCORE)
        near_top = near_stats[:, 0:1]
        top = jnp.maximum(near_top, jnp.maximum(mid_top, far_top))
        far_factor = jnp.exp(far_top - top)
        mid_factor = jnp.exp(mid_top - top)
        near_factor = jnp.exp(near_top - top)
        total = (
            near_factor * near_stats[:, 1:2]
            + mid_factor * mid_stats[:, 1:2]
            + far_factor * far_stats[:, 1:2]
        )
        far_factor = far_factor / total
        mid_factor = mid_factor / total
        near_factor = near_factor / total
        delta = (
            near_factor * near_stats[:, 2:3]
            + mid_factor * mid_stats[:, 2:3]
            + far_factor * far_stats[:, 2:3]
        )
        back = jnp.where(lanes == 0, far_factor, jnp.where(lanes == 1, mid_factor, delta))
        far_back = dot(chooser(FAR_ROWS, SPACING_WIDE, far_off), back, 1, 0)
        mid_back = dot(chooser(MID_ROWS, SPACING_CENTRAL, mid_off), back, 1, 0)
        near = branch_grads(near_in[j], near_factor, delta)
        mid = branch_grads(mid_start, mid_back[:, 1:2], mid_back[:, 2:3])
        far = branch_grads(far_in[j], far_back[:, 0:1], far_back[:, 2:3])
        far_both[j] = far
        mid_both[j] = mid
        near_both[j] = near
        side = (
            query_side(near, near_pairs_of(near_own, near_other, j))
            + dot(mid_put, query_side(mid, mid_pairs), 1, 0)
            + dot(far_put, query_side(far, gathered(far_refs, head_slice(j, FAR_ROWS))), 1, 0)
        )
        turned = side.T
        dq_ref[HEAD * j : HEAD * (j + 1), :] = turned[:HEAD] * SCALE
        attended.append(turned[HEAD:])
    live = iota((HEAD * LOCAL_HEADS, TOKENS), 1) < count[0]
    rows = jnp.where(live, jnp.concatenate(attended, axis=0), 0.0)
    terms_ref[...] = dot3(w_ref[...], rows, 0, 0)
    columns = term_refs[0].shape[0]
    heads = terms_ref.shape[0] // columns
    group = base[0] // LOCAL_HEADS
    for k, ref in enumerate(term_refs):
        at = pl.multiple_of(columns * ((group + k) % heads), columns)
        ref[...] = terms_ref[pl.ds(at, columns), :]
    weight = dot3(rows, cot_ref[...], 1, 1)
    for b in range(weight.shape[1] // 128):
        weight_ref[columns * b : columns * (b + 1), :] = weight[:, 128 * b : 128 * b + 128]


def keys_body(far_both, mid_both, near_both, qf_ref, qm_ref, qn_ref, *outs):
    far_refs, mid_refs, near_refs = outs[:2], outs[2:4], outs[4:]
    for j in range(LOCAL_HEADS):
        for both, q_ref, refs, rows in (
            (mid_both, qm_ref, mid_refs, MID_ROWS),
            (far_both, qf_ref, far_refs, FAR_ROWS),
        ):
            sums = dot3(both[j], split_queries(q_ref[j]), 0, 0)
            half = sums.shape[0] // 2
            for i, ref in enumerate(refs):
                ref[:, head_slice(j, rows), :] = sums[half * i : half * (i + 1)].reshape(
                    half // rows, rows, 128
                )
        sums = dot3(near_both[j], split_queries(qn_ref[j]), 0, 0)
        for i, ref in enumerate(near_refs):
            ref[head_slice(j, TOKENS), :] = sums[TOKENS * i : TOKENS * (i + 1)]


def finish_body(base, far_ref, mid_ref, near_ref, other_ref, dk_ref, dv_ref):
    far_sum = far_ref[0, :FAR_BLOCK, :]
    for i in range(1, far_ref.shape[0]):
        far_sum = far_sum + far_ref[i, :FAR_BLOCK, :]
    mid_sum = mid_ref[0, :MID_BLOCK, :]
    for i in range(1, mid_ref.shape[0]):
        mid_sum = mid_sum + mid_ref[i, :MID_BLOCK, :]
    for j in range(LOCAL_HEADS):
        head = base[0] + j
        ns = slice(TOKENS * j, TOKENS * (j + 1))
        far_put = placer(FAR_ROWS, SPACING_WIDE, head % SPACING_WIDE)
        mid_put = placer(MID_ROWS, SPACING_CENTRAL, head % SPACING_CENTRAL)
        both = (
            near_ref[ns, :]
            + other_ref[ns, :]
            + dot(mid_put, mid_sum[MID_ROWS * j : MID_ROWS * (j + 1)], 1, 0)
            + dot(far_put, far_sum[FAR_ROWS * j : FAR_ROWS * (j + 1)], 1, 0)
        )
        turned = both.T
        dk_ref[HEAD * j : HEAD * (j + 1), :] = turned[:HEAD]
        dv_ref[HEAD * j : HEAD * (j + 1), :] = turned[HEAD:]


def exchange(pieces, axis):
    return lax.all_to_all(pieces, axis, 0, 0, tiled=True)


def to_all(piece, axis):
    return exchange(jnp.broadcast_to(piece, (lax.axis_size(axis), *piece.shape)), axis)


def shifted(x, axis, apart):
    size = lax.axis_size(axis)
    return lax.ppermute(x, axis, [(i, (i + apart) % size) for i in range(size)])


def on_device(queries, keys, values, counts, out_weight, cotangent):
    ny, nz, nzh, nzl = (lax.axis_size(axis) for axis in ("y", Z, "zh", "zl"))
    heads = lax.axis_size("h")
    columns, tokens = queries.shape
    base = (lax.axis_index("h") * LOCAL_HEADS).astype(jnp.int32).reshape(1)

    cots = [cotangent] + [shifted(cotangent, "h", k % heads) for k in range(1, 4)]
    far_out, mid_out, near_own = kernel_call(
        pack_body,
        (shaped(nz, FAR_BLOCK, 128), shaped(nzl, MID_BLOCK, 128), shaped(NEAR_BLOCK, 128)),
        (counts, base, keys, values),
        2,
    )
    near_other = shifted(near_own, "c", 1)
    far_line = exchange(far_out, Z)
    query_far, query_mid, query_near, full_cot = kernel_call(
        query_body,
        (
            shaped(LOCAL_HEADS, FAR_ROWS, 128),
            shaped(LOCAL_HEADS, MID_ROWS, 128),
            shaped(LOCAL_HEADS, TOKENS, 128),
            shaped(heads * columns, tokens),
        ),
        (counts, base, queries, out_weight, *cots),
        2,
    )
    mid_own = exchange(mid_out, "zl")
    far_plane = [far_line] + [shifted(far_line, "y", k) for k in range(1, ny)]
    far_blocks = far_plane + [shifted(x, "c", 1) for x in far_plane]
    far_keys = 2 * ny * nz * FAR_ROWS
    far_both, far_stats, near_both, near_stats = kernel_call(
        scores_body,
        (
            shaped(LOCAL_HEADS, 2 * FAR_ROWS, far_keys),
            shaped(LOCAL_HEADS, FAR_ROWS, 128),
            shaped(LOCAL_HEADS, 2 * TOKENS, 2 * TOKENS),
            shaped(LOCAL_HEADS, TOKENS, 128),
        ),
        (query_far, query_near, near_own, near_other, *far_blocks),
        0,
    )
    mid_other = shifted(mid_own, "c", 1)
    mid_keys = 2 * nzl * MID_ROWS
    query_grad, weight, far_both, mid_both, near_both, *terms = kernel_call(
        attention_body,
        (
            shaped(columns, tokens),
            shaped(out_weight.size // 128, 128),
            shaped(LOCAL_HEADS, 2 * FAR_ROWS, far_keys),
            shaped(LOCAL_HEADS, 2 * MID_ROWS, mid_keys),
            shaped(LOCAL_HEADS, 2 * TOKENS, 2 * TOKENS),
        )
        + (shaped(columns, tokens),) * 4
        + (shaped(heads * columns, tokens),),
        (
            counts,
            base,
            query_mid,
            near_own,
            near_other,
            mid_own,
            mid_other,
            out_weight,
            full_cot,
            far_both,
            far_stats,
            near_both,
            near_stats,
            *far_blocks,
        ),
        2,
    )
    planes = 2 * ny
    weight_parts = exchange(weight.reshape(planes, -1, 128), ("y", "c"))
    far_keep, far_send, mid_keep, mid_send, near_keep, near_send = kernel_call(
        keys_body,
        (shaped(ny * nz, FAR_BLOCK, 128),) * 2
        + (shaped(nzl, MID_BLOCK, 128),) * 2
        + (shaped(NEAR_BLOCK, 128),) * 2,
        (far_both, mid_both, near_both, query_far, query_mid, query_near),
        0,
    )
    mid_got = shifted(mid_send, "c", 1)
    weight_line = jnp.sum(weight_parts, axis=0).reshape(nzl, -1, 128)
    mid_sums = exchange(jnp.concatenate([mid_keep + mid_got, weight_line], axis=1), "zl")
    far_got = shifted(far_send, "c", 1)
    near_got = shifted(near_send, "c", 1)
    pieces = [far_keep[nz * k : nz * (k + 1)] + far_got[nz * k : nz * (k + 1)] for k in range(ny)]
    pieces = pieces[:1] + [shifted(pieces[k], "y", -k) for k in range(1, ny)]
    far_total = sum(pieces[1:], pieces[0])
    weight_own = jnp.sum(mid_sums[:, MID_BLOCK:], axis=0)
    depth = weight_own.shape[0]
    parts = exchange(
        jnp.concatenate(
            [far_total, jnp.broadcast_to(weight_own, (nz, depth, 128))], axis=1
        ),
        Z,
    )
    got = [terms[0]] + [shifted(terms[k], "h", k % heads) for k in range(1, 4)]
    output = sum(got[1:], got[0])
    weight_whole = jnp.sum(parts[:, FAR_BLOCK:].reshape(nzh, nzl, depth, 128), axis=0)
    weight_rows = to_all(weight_whole.reshape(nzl * depth, 128), ("y", "c"))
    weight_grad = (
        weight_rows.reshape(out_weight.shape[1] // 128, out_weight.shape[0], 128)
        .swapaxes(0, 1)
        .reshape(out_weight.shape)
    )
    key_grad, value_grad = kernel_call(
        finish_body,
        (shaped(columns, tokens), shaped(columns, tokens)),
        (base, parts, mid_sums, near_keep, near_got),
        1,
    )
    return output, query_grad, key_grad, value_grad, weight_grad


def solution(mesh):
    split = Mesh(
        mesh.devices.reshape(4, 2, 8, 2, mesh.shape["head"]), ("y", "zh", "zl", "c", "h")
    )
    return on_mesh(split)


def on_mesh(split):
    in_specs = (
        P("h", SEQ),
        P("h", SEQ),
        P("h", SEQ),
        P(SEQ),
        P("h", None),
        P("h", SEQ),
    )
    out_specs = (P("h", SEQ), P("h", SEQ), P("h", SEQ), P("h", SEQ), P("h", None))
    return jax.shard_map(
        on_device, mesh=split, in_specs=in_specs, out_specs=out_specs, check_vma=False
    )
```

```python
import jax
import jax.numpy as jnp
from jax import lax
from jax.experimental import pallas as pl
from jax.experimental.pallas import tpu as pltpu
from jax.sharding import Mesh
from jax.sharding import PartitionSpec as P

HEAD = 64
LOCAL_HEADS = 3
TOKENS = 128
SPACING_CENTRAL = 4
SPACING_WIDE = 16
MID_ROWS = TOKENS // SPACING_CENTRAL
FAR_ROWS = TOKENS // SPACING_WIDE
FAR_BLOCK = LOCAL_HEADS * FAR_ROWS
MID_BLOCK = LOCAL_HEADS * MID_ROWS
NEAR_BLOCK = LOCAL_HEADS * TOKENS
SCALE = HEAD ** (-0.5)
MASKED_SCORE = -1e30
DEAD_MARK = 1e6
DEAD_LEVEL = 1e5
INTERPRET = False
SEQ = ("y", "zh", "zl", "c")
Z = ("zh", "zl")


def dot(a, b, ca, cb):
    return lax.dot_general(
        a,
        b,
        (((ca,), (cb,)), ((), ())),
        precision=lax.Precision.HIGHEST,
        preferred_element_type=jnp.float32,
    )


def halves(x):
    high = x.astype(jnp.bfloat16)
    return high, (x - high.astype(jnp.float32)).astype(jnp.bfloat16)


def dot3(a, b, ca, cb):
    a_high, a_low = halves(a)
    b_high, b_low = halves(b)

    def one(x, y):
        return lax.dot_general(
            x, y, (((ca,), (cb,)), ((), ())), preferred_element_type=jnp.float32
        )

    return one(a_low, b_high) + one(a_high, b_low) + one(a_high, b_high)


def iota(shape, dim):
    return lax.broadcasted_iota(jnp.int32, shape, dim)


def chooser(rows, spacing, offset):
    shape = (rows, TOKENS)
    return (iota(shape, 1) == iota(shape, 0) * spacing + offset).astype(jnp.float32)


def placer(rows, spacing, offset):
    shape = (TOKENS, rows)
    return (iota(shape, 0) == iota(shape, 1) * spacing + offset).astype(jnp.float32)


def kernel_call(body, out_shape, operands, scalars):
    in_specs = [pl.BlockSpec(memory_space=pltpu.SMEM)] * scalars + [
        pl.BlockSpec(memory_space=pltpu.VMEM)
    ] * (len(operands) - scalars)
    return pl.pallas_call(
        body,
        out_shape=out_shape,
        in_specs=in_specs,
        out_specs=jax.tree.map(lambda _: pl.BlockSpec(memory_space=pltpu.VMEM), out_shape),
        interpret=INTERPRET,
    )(*operands)


def shaped(*dims):
    return jax.ShapeDtypeStruct(dims, jnp.float32)


def pack_body(count, base, k_ref, v_ref, far_ref, mid_ref, near_ref):
    feature = iota((2 * HEAD, TOKENS), 0)
    live = iota((2 * HEAD, TOKENS), 1) < count[0]
    for j in range(LOCAL_HEADS):
        rows = slice(HEAD * j, HEAD * (j + 1))
        both = jnp.concatenate([k_ref[rows, :], v_ref[rows, :]], axis=0)
        both = jnp.where(live, both, jnp.where(feature == 0, DEAD_MARK, 0.0))
        turned = both.T
        near_ref[TOKENS * j : TOKENS * (j + 1), :] = turned
        head = base[0] + j
        far = dot(chooser(FAR_ROWS, SPACING_WIDE, head % SPACING_WIDE), turned, 1, 0)
        mid = dot(chooser(MID_ROWS, SPACING_CENTRAL, head % SPACING_CENTRAL), turned, 1, 0)
        for i in range(far_ref.shape[0]):
            far_ref[i, FAR_ROWS * j : FAR_ROWS * (j + 1), :] = far
        for i in range(mid_ref.shape[0]):
            mid_ref[i, MID_ROWS * j : MID_ROWS * (j + 1), :] = mid


def query_body(count, base, q_ref, w_ref, cot_ref, far_ref, mid_ref, near_ref):
    live = iota((HEAD, TOKENS), 1) < count[0]
    grads = dot3(w_ref[...], cot_ref[...], 1, 0)
    for j in range(LOCAL_HEADS):
        rows = slice(HEAD * j, HEAD * (j + 1))
        both = jnp.concatenate(
            [q_ref[rows, :] * SCALE, jnp.where(live, grads[rows, :], 0.0)], axis=0
        )
        turned = both.T
        head = base[0] + j
        near_ref[j] = turned
        far_ref[j] = dot(chooser(FAR_ROWS, SPACING_WIDE, head % SPACING_WIDE), turned, 1, 0)
        mid_ref[j] = dot(
            chooser(MID_ROWS, SPACING_CENTRAL, head % SPACING_CENTRAL), turned, 1, 0
        )


def split_queries(turned):
    left = iota(turned.shape, 1) < HEAD
    return jnp.concatenate([jnp.where(left, turned, 0.0), jnp.where(left, 0.0, turned)], axis=0)


def branch_scores(turned, pairs):
    rows = turned.shape[0]
    mark = ((iota((8, 2 * HEAD), 0) == 0) & (iota((8, 2 * HEAD), 1) == 0)).astype(jnp.float32)
    products = dot3(jnp.concatenate([split_queries(turned), mark], axis=0), pairs, 1, 1)
    dead = products[2 * rows : 2 * rows + 1, :] > DEAD_LEVEL
    scores = jnp.where(dead, MASKED_SCORE, products[:rows])
    prob_grads = products[rows : 2 * rows]
    top = jnp.max(scores, axis=1, keepdims=True)
    weights = jnp.exp(scores - top)
    total = jnp.sum(weights, axis=1, keepdims=True)
    pulled = jnp.sum(weights * prob_grads, axis=1, keepdims=True)
    at = iota((rows, 128), 1)
    stats = jnp.where(at == 0, top, jnp.where(at == 1, total, pulled))
    return jnp.concatenate([prob_grads, weights], axis=0), stats


def branch_grads(both, factor, delta):
    rows = both.shape[0] // 2
    probs = both[rows:] * factor
    return jnp.concatenate([probs * (both[:rows] - delta), probs], axis=0)


def query_side(both, pairs):
    rows = both.shape[0] // 2
    sums = dot3(both, pairs, 1, 0)
    left = iota((rows, 2 * HEAD), 1) < HEAD
    return jnp.where(left, sums[:rows], sums[rows:])


def gathered(refs, rows):
    parts = []
    for ref in refs:
        part = ref[:, rows, :]
        parts.append(part.reshape(part.shape[0] * part.shape[1], 128))
    return jnp.concatenate(parts, axis=0)


def head_slice(j, rows):
    return slice(rows * j, rows * (j + 1))


def near_pairs_of(own, other, j):
    rows = head_slice(j, TOKENS)
    return jnp.concatenate([own[rows, :], other[rows, :]], axis=0)


def near_scores_body(q_ref, near_own, near_other, both_ref, stats_ref):
    for j in range(LOCAL_HEADS):
        pairs = near_pairs_of(near_own, near_other, j)
        both_ref[j], stats_ref[j] = branch_scores(q_ref[j], pairs)


def far_scores_body(q_ref, far_own, far_other, both_ref, stats_ref):
    for j in range(LOCAL_HEADS):
        pairs = gathered((far_own, far_other), head_slice(j, FAR_ROWS))
        both_ref[j], stats_ref[j] = branch_scores(q_ref[j], pairs)


def attention_body(*refs):
    count, base = refs[:2]
    qm_ref, near_own, near_other, mid_own, mid_other, cot_ref = refs[2:8]
    far_in, far_stats_ref, near_in, near_stats_ref = refs[8:12]
    far_refs = refs[12:14]
    dq_ref, attended_ref, weight_ref, far_both, mid_both, near_both = refs[14:]
    lanes = iota((TOKENS, 128), 1)
    position = iota((TOKENS, 1), 0)
    attended = []
    for j in range(LOCAL_HEADS):
        head = base[0] + j
        far_off = head % SPACING_WIDE
        mid_off = head % SPACING_CENTRAL
        mid_pairs = gathered((mid_own, mid_other), head_slice(j, MID_ROWS))
        mid_start, mid_column = branch_scores(qm_ref[j], mid_pairs)
        far_put = placer(FAR_ROWS, SPACING_WIDE, far_off)
        mid_put = placer(MID_ROWS, SPACING_CENTRAL, mid_off)
        far_stats = dot(far_put, far_stats_ref[j], 1, 0)
        mid_stats = dot(mid_put, mid_column, 1, 0)
        near_stats = near_stats_ref[j]
        in_far = position % SPACING_WIDE == far_off
        in_mid = position % SPACING_CENTRAL == mid_off
        far_top = jnp.where(in_far, far_stats[:, 0:1], MASKED_SCORE)
        mid_top = jnp.where(in_mid, mid_stats[:, 0:1], MASKED_SCORE)
        near_top = near_stats[:, 0:1]
        top = jnp.maximum(near_top, jnp.maximum(mid_top, far_top))
        far_factor = jnp.exp(far_top - top)
        mid_factor = jnp.exp(mid_top - top)
        near_factor = jnp.exp(near_top - top)
        total = (
            near_factor * near_stats[:, 1:2]
            + mid_factor * mid_stats[:, 1:2]
            + far_factor * far_stats[:, 1:2]
        )
        far_factor = far_factor / total
        mid_factor = mid_factor / total
        near_factor = near_factor / total
        delta = (
            near_factor * near_stats[:, 2:3]
            + mid_factor * mid_stats[:, 2:3]
            + far_factor * far_stats[:, 2:3]
        )
        back = jnp.where(lanes == 0, far_factor, jnp.where(lanes == 1, mid_factor, delta))
        far_back = dot(chooser(FAR_ROWS, SPACING_WIDE, far_off), back, 1, 0)
        mid_back = dot(chooser(MID_ROWS, SPACING_CENTRAL, mid_off), back, 1, 0)
        near = branch_grads(near_in[j], near_factor, delta)
        mid = branch_grads(mid_start, mid_back[:, 1:2], mid_back[:, 2:3])
        far = branch_grads(far_in[j], far_back[:, 0:1], far_back[:, 2:3])
        far_both[j] = far
        mid_both[j] = mid
        near_both[j] = near
        side = (
            query_side(near, near_pairs_of(near_own, near_other, j))
            + dot(mid_put, query_side(mid, mid_pairs), 1, 0)
            + dot(far_put, query_side(far, gathered(far_refs, head_slice(j, FAR_ROWS))), 1, 0)
        )
        turned = side.T
        dq_ref[HEAD * j : HEAD * (j + 1), :] = turned[:HEAD] * SCALE
        attended.append(turned[HEAD:])
    live = iota((HEAD * LOCAL_HEADS, TOKENS), 1) < count[0]
    rows = jnp.where(live, jnp.concatenate(attended, axis=0), 0.0)
    attended_ref[...] = rows
    columns = rows.shape[0]
    weight = dot3(rows, cot_ref[...], 1, 1)
    for b in range(weight.shape[1] // 128):
        weight_ref[columns * b : columns * (b + 1), :] = weight[:, 128 * b : 128 * b + 128]


def terms_body(base, attended_ref, w_ref, *refs):
    term_refs, terms_ref = refs[:4], refs[4]
    terms_ref[...] = dot3(w_ref[...], attended_ref[...], 0, 0)
    columns = term_refs[0].shape[0]
    heads = terms_ref.shape[0] // columns
    group = base[0] // LOCAL_HEADS
    for k, ref in enumerate(term_refs):
        at = pl.multiple_of(columns * ((group + k) % heads), columns)
        ref[...] = terms_ref[pl.ds(at, columns), :]


def wide_keys(both, turned, refs, j):
    sums = dot3(both, split_queries(turned), 0, 0)
    rows = turned.shape[0]
    half = sums.shape[0] // 2
    for i, ref in enumerate(refs):
        ref[:, head_slice(j, rows), :] = sums[half * i : half * (i + 1)].reshape(
            half // rows, rows, 128
        )


def mid_keys_body(both_ref, q_ref, *refs):
    for j in range(LOCAL_HEADS):
        wide_keys(both_ref[j], q_ref[j], refs, j)


def keys_body(far_both, near_both, qf_ref, qn_ref, *outs):
    for j in range(LOCAL_HEADS):
        wide_keys(far_both[j], qf_ref[j], outs[:2], j)
        sums = dot3(near_both[j], split_queries(qn_ref[j]), 0, 0)
        for i, ref in enumerate(outs[2:]):
            ref[head_slice(j, TOKENS), :] = sums[TOKENS * i : TOKENS * (i + 1)]


def total_of(ref):
    total = ref[0]
    for i in range(1, ref.shape[0]):
        total = total + ref[i]
    return total


def mid_join_body(keep_ref, got_ref, weight_ref, out_ref):
    weight = total_of(weight_ref)
    depth = weight.shape[0] // out_ref.shape[0]
    for i in range(out_ref.shape[0]):
        out_ref[i, :MID_BLOCK, :] = keep_ref[i] + got_ref[i]
        out_ref[i, MID_BLOCK:, :] = weight[depth * i : depth * (i + 1)]


def far_join_body(mid_ref, *refs):
    out_ref = refs[-1]
    weight = mid_ref[0, MID_BLOCK:, :]
    for i in range(1, mid_ref.shape[0]):
        weight = weight + mid_ref[i, MID_BLOCK:, :]
    for i in range(out_ref.shape[0]):
        total = refs[0][i]
        for ref in refs[1:-1]:
            total = total + ref[i]
        out_ref[i, :FAR_BLOCK, :] = total
        out_ref[i, FAR_BLOCK:, :] = weight


def weight_join_body(far_ref, out_ref):
    lines = out_ref.shape[1] // (far_ref.shape[1] - FAR_BLOCK)
    depth = out_ref.shape[1] // lines
    for i in range(lines):
        total = far_ref[i, FAR_BLOCK:, :]
        for at in range(i + lines, far_ref.shape[0], lines):
            total = total + far_ref[at, FAR_BLOCK:, :]
        for to in range(out_ref.shape[0]):
            out_ref[to, depth * i : depth * (i + 1), :] = total


def finish_body(base, far_ref, mid_ref, near_ref, other_ref, dk_ref, dv_ref):
    far_sum = far_ref[0, :FAR_BLOCK, :]
    for i in range(1, far_ref.shape[0]):
        far_sum = far_sum + far_ref[i, :FAR_BLOCK, :]
    mid_sum = mid_ref[0, :MID_BLOCK, :]
    for i in range(1, mid_ref.shape[0]):
        mid_sum = mid_sum + mid_ref[i, :MID_BLOCK, :]
    for j in range(LOCAL_HEADS):
        head = base[0] + j
        ns = slice(TOKENS * j, TOKENS * (j + 1))
        far_put = placer(FAR_ROWS, SPACING_WIDE, head % SPACING_WIDE)
        mid_put = placer(MID_ROWS, SPACING_CENTRAL, head % SPACING_CENTRAL)
        both = (
            near_ref[ns, :]
            + other_ref[ns, :]
            + dot(mid_put, mid_sum[MID_ROWS * j : MID_ROWS * (j + 1)], 1, 0)
            + dot(far_put, far_sum[FAR_ROWS * j : FAR_ROWS * (j + 1)], 1, 0)
        )
        turned = both.T
        dk_ref[HEAD * j : HEAD * (j + 1), :] = turned[:HEAD]
        dv_ref[HEAD * j : HEAD * (j + 1), :] = turned[HEAD:]


def weight_order_body(in_ref, out_ref):
    rows = out_ref.shape[0]
    every = in_ref[...].reshape(in_ref.shape[0] * in_ref.shape[1], 128)
    for b in range(out_ref.shape[1] // 128):
        out_ref[:, 128 * b : 128 * b + 128] = every[rows * b : rows * (b + 1)]


def exchange(pieces, axis):
    return lax.all_to_all(pieces, axis, 0, 0, tiled=True)


def to_all(piece, axis):
    return exchange(jnp.broadcast_to(piece, (lax.axis_size(axis), *piece.shape)), axis)


def shifted(x, axis, apart):
    size = lax.axis_size(axis)
    return lax.ppermute(x, axis, [(i, (i + apart) % size) for i in range(size)])


def on_device(queries, keys, values, counts, out_weight, cotangent):
    ny, nz, _, nzl = (lax.axis_size(axis) for axis in ("y", Z, "zh", "zl"))
    heads = lax.axis_size("h")
    columns, tokens = queries.shape
    base = (lax.axis_index("h") * LOCAL_HEADS).astype(jnp.int32).reshape(1)

    full_cot = to_all(cotangent, "h").reshape(heads * columns, tokens)
    far_out, mid_out, near_own = kernel_call(
        pack_body,
        (shaped(nz, FAR_BLOCK, 128), shaped(nzl, MID_BLOCK, 128), shaped(NEAR_BLOCK, 128)),
        (counts, base, keys, values),
        2,
    )
    near_other = shifted(near_own, "c", 1)
    far_line = exchange(far_out, Z)
    query_far, query_mid, query_near = kernel_call(
        query_body,
        (
            shaped(LOCAL_HEADS, FAR_ROWS, 128),
            shaped(LOCAL_HEADS, MID_ROWS, 128),
            shaped(LOCAL_HEADS, TOKENS, 128),
        ),
        (counts, base, queries, out_weight, full_cot),
        2,
    )
    near_both, near_stats = kernel_call(
        near_scores_body,
        (shaped(LOCAL_HEADS, 2 * TOKENS, 2 * TOKENS), shaped(LOCAL_HEADS, TOKENS, 128)),
        (query_near, near_own, near_other),
        0,
    )
    mid_own = exchange(mid_out, "zl")
    far_own = jnp.concatenate(
        [far_line] + [shifted(far_line, "y", k) for k in range(1, ny)], axis=0
    )
    far_other = shifted(far_own, "c", 1)
    far_keys = 2 * ny * nz * FAR_ROWS
    far_both, far_stats = kernel_call(
        far_scores_body,
        (shaped(LOCAL_HEADS, 2 * FAR_ROWS, far_keys), shaped(LOCAL_HEADS, FAR_ROWS, 128)),
        (query_far, far_own, far_other),
        0,
    )
    mid_other = shifted(mid_own, "c", 1)
    mid_keys = 2 * nzl * MID_ROWS
    query_grad, attended, weight, far_both, mid_both, near_both = kernel_call(
        attention_body,
        (
            shaped(columns, tokens),
            shaped(columns, tokens),
            shaped(out_weight.size // 128, 128),
            shaped(LOCAL_HEADS, 2 * FAR_ROWS, far_keys),
            shaped(LOCAL_HEADS, 2 * MID_ROWS, mid_keys),
            shaped(LOCAL_HEADS, 2 * TOKENS, 2 * TOKENS),
        ),
        (
            counts,
            base,
            query_mid,
            near_own,
            near_other,
            mid_own,
            mid_other,
            full_cot,
            far_both,
            far_stats,
            near_both,
            near_stats,
            far_own,
            far_other,
        ),
        2,
    )
    planes = 2 * ny
    weight_parts = exchange(weight.reshape(planes, -1, 128), ("y", "c"))
    mid_keep, mid_send = kernel_call(
        mid_keys_body, (shaped(nzl, MID_BLOCK, 128),) * 2, (mid_both, query_mid), 0
    )
    mid_got = shifted(mid_send, "c", 1)
    depth = weight.shape[0] // (planes * nzl)
    mid_join = kernel_call(
        mid_join_body, shaped(nzl, MID_BLOCK + depth, 128), (mid_keep, mid_got, weight_parts), 0
    )
    mid_sums = exchange(mid_join, "zl")
    far_keep, far_send, near_keep, near_send = kernel_call(
        keys_body,
        (shaped(ny * nz, FAR_BLOCK, 128),) * 2 + (shaped(NEAR_BLOCK, 128),) * 2,
        (far_both, near_both, query_far, query_near),
        0,
    )
    far_got = shifted(far_send, "c", 1)
    near_got = shifted(near_send, "c", 1)
    pieces = [far_keep[nz * k : nz * (k + 1)] + far_got[nz * k : nz * (k + 1)] for k in range(ny)]
    pieces = pieces[:1] + [shifted(pieces[k], "y", -k) for k in range(1, ny)]
    far_join = kernel_call(
        far_join_body, shaped(nz, FAR_BLOCK + depth, 128), (mid_sums, *pieces), 0
    )
    parts = exchange(far_join, Z)
    terms = kernel_call(
        terms_body,
        (shaped(columns, tokens),) * 4 + (shaped(heads * columns, tokens),),
        (base, attended, out_weight),
        1,
    )
    got = [terms[0]] + [shifted(terms[k], "h", k % heads) for k in range(1, 4)]
    output = sum(got[1:], got[0])
    weight_rows = exchange(
        kernel_call(weight_join_body, shaped(planes, nzl * depth, 128), (parts,), 0), ("y", "c")
    )
    weight_grad = kernel_call(weight_order_body, shaped(*out_weight.shape), (weight_rows,), 0)
    key_grad, value_grad = kernel_call(
        finish_body,
        (shaped(columns, tokens), shaped(columns, tokens)),
        (base, parts, mid_sums, near_keep, near_got),
        1,
    )
    return output, query_grad, key_grad, value_grad, weight_grad


def solution(mesh):
    split = Mesh(
        mesh.devices.reshape(4, 2, 8, 2, mesh.shape["head"]), ("y", "zh", "zl", "c", "h")
    )
    return on_mesh(split)


def on_mesh(split):
    in_specs = (
        P("h", SEQ),
        P("h", SEQ),
        P("h", SEQ),
        P(SEQ),
        P("h", None),
        P("h", SEQ),
    )
    out_specs = (P("h", SEQ), P("h", SEQ), P("h", SEQ), P("h", SEQ), P("h", None))
    return jax.shard_map(
        on_device, mesh=split, in_specs=in_specs, out_specs=out_specs, check_vma=False
    )
```

```python
import jax
import jax.numpy as jnp
from jax import lax
from jax.experimental import pallas as pl
from jax.experimental.pallas import tpu as pltpu
from jax.sharding import Mesh
from jax.sharding import PartitionSpec as P

HEAD = 64
LOCAL_HEADS = 3
TOKENS = 128
SPACING_CENTRAL = 4
SPACING_WIDE = 16
MID_ROWS = TOKENS // SPACING_CENTRAL
FAR_ROWS = TOKENS // SPACING_WIDE
FAR_BLOCK = LOCAL_HEADS * FAR_ROWS
MID_BLOCK = LOCAL_HEADS * MID_ROWS
NEAR_BLOCK = LOCAL_HEADS * TOKENS
SCALE = HEAD ** (-0.5)
MASKED_SCORE = -1e30
DEAD_MARK = 1e6
DEAD_LEVEL = 1e5
INTERPRET = False
SEQ = ("y", "zh", "zl", "c")
Z = ("zh", "zl")


def dot(a, b, ca, cb):
    return lax.dot_general(
        a,
        b,
        (((ca,), (cb,)), ((), ())),
        precision=lax.Precision.HIGHEST,
        preferred_element_type=jnp.float32,
    )


def halves(x):
    high = x.astype(jnp.bfloat16)
    return high, (x - high.astype(jnp.float32)).astype(jnp.bfloat16)


def dot3(a, b, ca, cb):
    a_high, a_low = halves(a)
    b_high, b_low = halves(b)

    def one(x, y):
        return lax.dot_general(
            x, y, (((ca,), (cb,)), ((), ())), preferred_element_type=jnp.float32
        )

    return one(a_low, b_high) + one(a_high, b_low) + one(a_high, b_high)


def iota(shape, dim):
    return lax.broadcasted_iota(jnp.int32, shape, dim)


def chooser(rows, spacing, offset):
    shape = (rows, TOKENS)
    return (iota(shape, 1) == iota(shape, 0) * spacing + offset).astype(jnp.float32)


def placer(rows, spacing, offset):
    shape = (TOKENS, rows)
    return (iota(shape, 0) == iota(shape, 1) * spacing + offset).astype(jnp.float32)


def kernel_call(body, out_shape, operands, scalars):
    in_specs = [pl.BlockSpec(memory_space=pltpu.SMEM)] * scalars + [
        pl.BlockSpec(memory_space=pltpu.VMEM)
    ] * (len(operands) - scalars)
    return pl.pallas_call(
        body,
        out_shape=out_shape,
        in_specs=in_specs,
        out_specs=jax.tree.map(lambda _: pl.BlockSpec(memory_space=pltpu.VMEM), out_shape),
        interpret=INTERPRET,
    )(*operands)


def shaped(*dims):
    return jax.ShapeDtypeStruct(dims, jnp.float32)


def pack_body(count, base, k_ref, v_ref, far_ref, mid_ref, near_ref):
    feature = iota((2 * HEAD, TOKENS), 0)
    live = iota((2 * HEAD, TOKENS), 1) < count[0]
    for j in range(LOCAL_HEADS):
        rows = slice(HEAD * j, HEAD * (j + 1))
        both = jnp.concatenate([k_ref[rows, :], v_ref[rows, :]], axis=0)
        both = jnp.where(live, both, jnp.where(feature == 0, DEAD_MARK, 0.0))
        turned = both.T
        near_ref[TOKENS * j : TOKENS * (j + 1), :] = turned
        head = base[0] + j
        far = dot(chooser(FAR_ROWS, SPACING_WIDE, head % SPACING_WIDE), turned, 1, 0)
        mid = dot(chooser(MID_ROWS, SPACING_CENTRAL, head % SPACING_CENTRAL), turned, 1, 0)
        for i in range(far_ref.shape[0]):
            far_ref[i, FAR_ROWS * j : FAR_ROWS * (j + 1), :] = far
        for i in range(mid_ref.shape[0]):
            mid_ref[i, MID_ROWS * j : MID_ROWS * (j + 1), :] = mid


def query_body(count, base, q_ref, w_ref, own_ref, one_ref, two_ref, three_ref, *outs):
    far_ref, mid_ref, near_ref, cot_ref = outs
    columns = own_ref.shape[0]
    heads = cot_ref.shape[0] // columns
    group = base[0] // LOCAL_HEADS
    for k, ref in enumerate((own_ref, one_ref, two_ref, three_ref)):
        at = pl.multiple_of(columns * ((group + heads - k) % heads), columns)
        cot_ref[pl.ds(at, columns), :] = ref[...]
    live = iota((HEAD, TOKENS), 1) < count[0]
    grads = dot3(w_ref[...], cot_ref[...], 1, 0)
    for j in range(LOCAL_HEADS):
        rows = slice(HEAD * j, HEAD * (j + 1))
        both = jnp.concatenate(
            [q_ref[rows, :] * SCALE, jnp.where(live, grads[rows, :], 0.0)], axis=0
        )
        turned = both.T
        head = base[0] + j
        near_ref[j] = turned
        far_ref[j] = dot(chooser(FAR_ROWS, SPACING_WIDE, head % SPACING_WIDE), turned, 1, 0)
        mid_ref[j] = dot(
            chooser(MID_ROWS, SPACING_CENTRAL, head % SPACING_CENTRAL), turned, 1, 0
        )


def split_queries(turned):
    left = iota(turned.shape, 1) < HEAD
    return jnp.concatenate([jnp.where(left, turned, 0.0), jnp.where(left, 0.0, turned)], axis=0)


def branch_scores(turned, pairs):
    rows = turned.shape[0]
    mark = ((iota((8, 2 * HEAD), 0) == 0) & (iota((8, 2 * HEAD), 1) == 0)).astype(jnp.float32)
    products = dot3(jnp.concatenate([split_queries(turned), mark], axis=0), pairs, 1, 1)
    dead = products[2 * rows : 2 * rows + 1, :] > DEAD_LEVEL
    scores = jnp.where(dead, MASKED_SCORE, products[:rows])
    prob_grads = products[rows : 2 * rows]
    top = jnp.max(scores, axis=1, keepdims=True)
    weights = jnp.exp(scores - top)
    total = jnp.sum(weights, axis=1, keepdims=True)
    pulled = jnp.sum(weights * prob_grads, axis=1, keepdims=True)
    at = iota((rows, 128), 1)
    stats = jnp.where(at == 0, top, jnp.where(at == 1, total, pulled))
    return jnp.concatenate([prob_grads, weights], axis=0), stats


def branch_grads(both, factor, delta):
    rows = both.shape[0] // 2
    probs = both[rows:] * factor
    return jnp.concatenate([probs * (both[:rows] - delta), probs], axis=0)


def query_side(both, pairs):
    rows = both.shape[0] // 2
    sums = dot3(both, pairs, 1, 0)
    left = iota((rows, 2 * HEAD), 1) < HEAD
    return jnp.where(left, sums[:rows], sums[rows:])


def gathered(refs, rows):
    parts = []
    for ref in refs:
        part = ref[:, rows, :]
        parts.append(part.reshape(part.shape[0] * part.shape[1], 128))
    return jnp.concatenate(parts, axis=0)


def head_slice(j, rows):
    return slice(rows * j, rows * (j + 1))


def near_pairs_of(own, other, j):
    rows = head_slice(j, TOKENS)
    return jnp.concatenate([own[rows, :], other[rows, :]], axis=0)


def near_scores_body(q_ref, near_own, near_other, both_ref, stats_ref):
    for j in range(LOCAL_HEADS):
        pairs = near_pairs_of(near_own, near_other, j)
        both_ref[j], stats_ref[j] = branch_scores(q_ref[j], pairs)


def far_scores_body(q_ref, far_own, far_other, both_ref, stats_ref):
    for j in range(LOCAL_HEADS):
        pairs = gathered((far_own, far_other), head_slice(j, FAR_ROWS))
        both_ref[j], stats_ref[j] = branch_scores(q_ref[j], pairs)


def attention_body(*refs):
    count, base = refs[:2]
    qm_ref, near_own, near_other, mid_own, mid_other, cot_ref = refs[2:8]
    far_in, far_stats_ref, near_in, near_stats_ref = refs[8:12]
    far_refs = refs[12:14]
    dq_ref, attended_ref, weight_ref, far_both, mid_both, near_both = refs[14:]
    lanes = iota((TOKENS, 128), 1)
    position = iota((TOKENS, 1), 0)
    attended = []
    for j in range(LOCAL_HEADS):
        head = base[0] + j
        far_off = head % SPACING_WIDE
        mid_off = head % SPACING_CENTRAL
        mid_pairs = gathered((mid_own, mid_other), head_slice(j, MID_ROWS))
        mid_start, mid_column = branch_scores(qm_ref[j], mid_pairs)
        far_put = placer(FAR_ROWS, SPACING_WIDE, far_off)
        mid_put = placer(MID_ROWS, SPACING_CENTRAL, mid_off)
        far_stats = dot(far_put, far_stats_ref[j], 1, 0)
        mid_stats = dot(mid_put, mid_column, 1, 0)
        near_stats = near_stats_ref[j]
        in_far = position % SPACING_WIDE == far_off
        in_mid = position % SPACING_CENTRAL == mid_off
        far_top = jnp.where(in_far, far_stats[:, 0:1], MASKED_SCORE)
        mid_top = jnp.where(in_mid, mid_stats[:, 0:1], MASKED_SCORE)
        near_top = near_stats[:, 0:1]
        top = jnp.maximum(near_top, jnp.maximum(mid_top, far_top))
        far_factor = jnp.exp(far_top - top)
        mid_factor = jnp.exp(mid_top - top)
        near_factor = jnp.exp(near_top - top)
        total = (
            near_factor * near_stats[:, 1:2]
            + mid_factor * mid_stats[:, 1:2]
            + far_factor * far_stats[:, 1:2]
        )
        far_factor = far_factor / total
        mid_factor = mid_factor / total
        near_factor = near_factor / total
        delta = (
            near_factor * near_stats[:, 2:3]
            + mid_factor * mid_stats[:, 2:3]
            + far_factor * far_stats[:, 2:3]
        )
        back = jnp.where(lanes == 0, far_factor, jnp.where(lanes == 1, mid_factor, delta))
        far_back = dot(chooser(FAR_ROWS, SPACING_WIDE, far_off), back, 1, 0)
        mid_back = dot(chooser(MID_ROWS, SPACING_CENTRAL, mid_off), back, 1, 0)
        near = branch_grads(near_in[j], near_factor, delta)
        mid = branch_grads(mid_start, mid_back[:, 1:2], mid_back[:, 2:3])
        far = branch_grads(far_in[j], far_back[:, 0:1], far_back[:, 2:3])
        far_both[j] = far
        mid_both[j] = mid
        near_both[j] = near
        side = (
            query_side(near, near_pairs_of(near_own, near_other, j))
            + dot(mid_put, query_side(mid, mid_pairs), 1, 0)
            + dot(far_put, query_side(far, gathered(far_refs, head_slice(j, FAR_ROWS))), 1, 0)
        )
        turned = side.T
        dq_ref[HEAD * j : HEAD * (j + 1), :] = turned[:HEAD] * SCALE
        attended.append(turned[HEAD:])
    live = iota((HEAD * LOCAL_HEADS, TOKENS), 1) < count[0]
    rows = jnp.where(live, jnp.concatenate(attended, axis=0), 0.0)
    attended_ref[...] = rows
    columns = rows.shape[0]
    weight = dot3(rows, cot_ref[...], 1, 1)
    for b in range(weight.shape[1] // 128):
        weight_ref[columns * b : columns * (b + 1), :] = weight[:, 128 * b : 128 * b + 128]


def terms_body(base, attended_ref, w_ref, *refs):
    term_refs, terms_ref = refs[:4], refs[4]
    terms_ref[...] = dot3(w_ref[...], attended_ref[...], 0, 0)
    columns = term_refs[0].shape[0]
    heads = terms_ref.shape[0] // columns
    group = base[0] // LOCAL_HEADS
    for k, ref in enumerate(term_refs):
        at = pl.multiple_of(columns * ((group + k) % heads), columns)
        ref[...] = terms_ref[pl.ds(at, columns), :]


def wide_keys(both, turned, refs, j):
    sums = dot3(both, split_queries(turned), 0, 0)
    rows = turned.shape[0]
    half = sums.shape[0] // 2
    for i, ref in enumerate(refs):
        ref[:, head_slice(j, rows), :] = sums[half * i : half * (i + 1)].reshape(
            half // rows, rows, 128
        )


def keys_body(far_both, mid_both, near_both, qf_ref, qm_ref, qn_ref, *outs):
    for j in range(LOCAL_HEADS):
        wide_keys(mid_both[j], qm_ref[j], outs[2:4], j)
        wide_keys(far_both[j], qf_ref[j], outs[:2], j)
        sums = dot3(near_both[j], split_queries(qn_ref[j]), 0, 0)
        for i, ref in enumerate(outs[4:]):
            ref[head_slice(j, TOKENS), :] = sums[TOKENS * i : TOKENS * (i + 1)]


def finish_body(base, far_ref, mid_ref, near_ref, other_ref, dk_ref, dv_ref):
    far_sum = far_ref[0, :FAR_BLOCK, :]
    for i in range(1, far_ref.shape[0]):
        far_sum = far_sum + far_ref[i, :FAR_BLOCK, :]
    mid_sum = mid_ref[0, :MID_BLOCK, :]
    for i in range(1, mid_ref.shape[0]):
        mid_sum = mid_sum + mid_ref[i, :MID_BLOCK, :]
    for j in range(LOCAL_HEADS):
        head = base[0] + j
        ns = slice(TOKENS * j, TOKENS * (j + 1))
        far_put = placer(FAR_ROWS, SPACING_WIDE, head % SPACING_WIDE)
        mid_put = placer(MID_ROWS, SPACING_CENTRAL, head % SPACING_CENTRAL)
        both = (
            near_ref[ns, :]
            + other_ref[ns, :]
            + dot(mid_put, mid_sum[MID_ROWS * j : MID_ROWS * (j + 1)], 1, 0)
            + dot(far_put, far_sum[FAR_ROWS * j : FAR_ROWS * (j + 1)], 1, 0)
        )
        turned = both.T
        dk_ref[HEAD * j : HEAD * (j + 1), :] = turned[:HEAD]
        dv_ref[HEAD * j : HEAD * (j + 1), :] = turned[HEAD:]


def exchange(pieces, axis):
    return lax.all_to_all(pieces, axis, 0, 0, tiled=True)


def to_all(piece, axis):
    return exchange(jnp.broadcast_to(piece, (lax.axis_size(axis), *piece.shape)), axis)


def shifted(x, axis, apart):
    size = lax.axis_size(axis)
    return lax.ppermute(x, axis, [(i, (i + apart) % size) for i in range(size)])


def on_device(queries, keys, values, counts, out_weight, cotangent):
    ny, nz, nzh, nzl = (lax.axis_size(axis) for axis in ("y", Z, "zh", "zl"))
    heads = lax.axis_size("h")
    columns, tokens = queries.shape
    base = (lax.axis_index("h") * LOCAL_HEADS).astype(jnp.int32).reshape(1)

    cots = [cotangent] + [shifted(cotangent, "h", k % heads) for k in range(1, 4)]
    far_out, mid_out, near_own = kernel_call(
        pack_body,
        (shaped(nz, FAR_BLOCK, 128), shaped(nzl, MID_BLOCK, 128), shaped(NEAR_BLOCK, 128)),
        (counts, base, keys, values),
        2,
    )
    near_other = shifted(near_own, "c", 1)
    far_line = exchange(far_out, Z)
    query_far, query_mid, query_near, full_cot = kernel_call(
        query_body,
        (
            shaped(LOCAL_HEADS, FAR_ROWS, 128),
            shaped(LOCAL_HEADS, MID_ROWS, 128),
            shaped(LOCAL_HEADS, TOKENS, 128),
            shaped(heads * columns, tokens),
        ),
        (counts, base, queries, out_weight, *cots),
        2,
    )
    near_both, near_stats = kernel_call(
        near_scores_body,
        (shaped(LOCAL_HEADS, 2 * TOKENS, 2 * TOKENS), shaped(LOCAL_HEADS, TOKENS, 128)),
        (query_near, near_own, near_other),
        0,
    )
    mid_own = exchange(mid_out, "zl")
    far_own = jnp.concatenate(
        [far_line] + [shifted(far_line, "y", k) for k in range(1, ny)], axis=0
    )
    far_other = shifted(far_own, "c", 1)
    far_keys = 2 * ny * nz * FAR_ROWS
    far_both, far_stats = kernel_call(
        far_scores_body,
        (shaped(LOCAL_HEADS, 2 * FAR_ROWS, far_keys), shaped(LOCAL_HEADS, FAR_ROWS, 128)),
        (query_far, far_own, far_other),
        0,
    )
    mid_other = shifted(mid_own, "c", 1)
    mid_keys = 2 * nzl * MID_ROWS
    query_grad, attended, weight, far_both, mid_both, near_both = kernel_call(
        attention_body,
        (
            shaped(columns, tokens),
            shaped(columns, tokens),
            shaped(out_weight.size // 128, 128),
            shaped(LOCAL_HEADS, 2 * FAR_ROWS, far_keys),
            shaped(LOCAL_HEADS, 2 * MID_ROWS, mid_keys),
            shaped(LOCAL_HEADS, 2 * TOKENS, 2 * TOKENS),
        ),
        (
            counts,
            base,
            query_mid,
            near_own,
            near_other,
            mid_own,
            mid_other,
            full_cot,
            far_both,
            far_stats,
            near_both,
            near_stats,
            far_own,
            far_other,
        ),
        2,
    )
    planes = 2 * ny
    weight_parts = exchange(weight.reshape(planes, -1, 128), ("y", "c"))
    far_keep, far_send, mid_keep, mid_send, near_keep, near_send = kernel_call(
        keys_body,
        (shaped(ny * nz, FAR_BLOCK, 128),) * 2
        + (shaped(nzl, MID_BLOCK, 128),) * 2
        + (shaped(NEAR_BLOCK, 128),) * 2,
        (far_both, mid_both, near_both, query_far, query_mid, query_near),
        0,
    )
    mid_got = shifted(mid_send, "c", 1)
    weight_line = jnp.sum(weight_parts, axis=0).reshape(nzl, -1, 128)
    mid_sums = exchange(jnp.concatenate([mid_keep + mid_got, weight_line], axis=1), "zl")
    far_got = shifted(far_send, "c", 1)
    near_got = shifted(near_send, "c", 1)
    pieces = [far_keep[nz * k : nz * (k + 1)] + far_got[nz * k : nz * (k + 1)] for k in range(ny)]
    pieces = pieces[:1] + [shifted(pieces[k], "y", -k) for k in range(1, ny)]
    far_total = sum(pieces[1:], pieces[0])
    weight_own = jnp.sum(mid_sums[:, MID_BLOCK:], axis=0)
    depth = weight_own.shape[0]
    parts = exchange(
        jnp.concatenate(
            [far_total, jnp.broadcast_to(weight_own, (nz, depth, 128))], axis=1
        ),
        Z,
    )
    terms = kernel_call(
        terms_body,
        (shaped(columns, tokens),) * 4 + (shaped(heads * columns, tokens),),
        (base, attended, out_weight),
        1,
    )
    got = [terms[0]] + [shifted(terms[k], "h", k % heads) for k in range(1, 4)]
    output = sum(got[1:], got[0])
    weight_whole = jnp.sum(parts[:, FAR_BLOCK:].reshape(nzh, nzl, depth, 128), axis=0)
    weight_rows = to_all(weight_whole.reshape(nzl * depth, 128), ("y", "c"))
    weight_grad = (
        weight_rows.reshape(out_weight.shape[1] // 128, out_weight.shape[0], 128)
        .swapaxes(0, 1)
        .reshape(out_weight.shape)
    )
    key_grad, value_grad = kernel_call(
        finish_body,
        (shaped(columns, tokens), shaped(columns, tokens)),
        (base, parts, mid_sums, near_keep, near_got),
        1,
    )
    return output, query_grad, key_grad, value_grad, weight_grad


def solution(mesh):
    split = Mesh(
        mesh.devices.reshape(4, 2, 8, 2, mesh.shape["head"]), ("y", "zh", "zl", "c", "h")
    )
    return on_mesh(split)


def on_mesh(split):
    in_specs = (
        P("h", SEQ),
        P("h", SEQ),
        P("h", SEQ),
        P(SEQ),
        P("h", None),
        P("h", SEQ),
    )
    out_specs = (P("h", SEQ), P("h", SEQ), P("h", SEQ), P("h", SEQ), P("h", None))
    return jax.shard_map(
        on_device, mesh=split, in_specs=in_specs, out_specs=out_specs, check_vma=False
    )
```

```python
import jax
import jax.numpy as jnp
from jax import lax
from jax.experimental import pallas as pl
from jax.experimental.pallas import tpu as pltpu
from jax.sharding import Mesh
from jax.sharding import PartitionSpec as P

HEAD = 64
LOCAL_HEADS = 3
TOKENS = 128
SPACING_CENTRAL = 4
SPACING_WIDE = 16
MID_ROWS = TOKENS // SPACING_CENTRAL
FAR_ROWS = TOKENS // SPACING_WIDE
FAR_BLOCK = LOCAL_HEADS * FAR_ROWS
MID_BLOCK = LOCAL_HEADS * MID_ROWS
NEAR_BLOCK = LOCAL_HEADS * TOKENS
SCALE = HEAD ** (-0.5)
MASKED_SCORE = -1e30
DEAD_MARK = 1e6
DEAD_LEVEL = 1e5
INTERPRET = False
SEQ = ("y", "zh", "zl", "c")
Z = ("zh", "zl")


def halves(x):
    high = x.astype(jnp.bfloat16)
    return high, (x - high.astype(jnp.float32)).astype(jnp.bfloat16)


def product(a, b, ca, cb):
    return lax.dot_general(
        a, b, (((ca,), (cb,)), ((), ())), preferred_element_type=jnp.float32
    )


def dot3(a, b, ca, cb):
    a_high, a_low = halves(a)
    b_high, b_low = halves(b)
    if ca == 1:
        rows = a.shape[0]
        both = product(jnp.concatenate([a_high, a_low], axis=0), b_high, ca, cb)
        return both[rows:] + product(a_high, b_low, ca, cb) + both[:rows]
    return product(a_low, b_high, ca, cb) + product(a_high, b_low, ca, cb) + product(a_high, b_high, ca, cb)


def outer3(a, b):
    a_high, a_low = halves(a)
    b_high, b_low = halves(b)
    return product(
        jnp.concatenate([a_low, a_high, a_high], axis=0),
        jnp.concatenate([b_high, b_low, b_high], axis=0),
        0,
        0,
    )


def iota(shape, dim):
    return lax.broadcasted_iota(jnp.int32, shape, dim)


def far_rows(j, head):
    return pl.ds(TOKENS * j + head % SPACING_WIDE, FAR_ROWS, stride=SPACING_WIDE)


def mid_rows(j, head):
    return pl.ds(TOKENS * j + head % SPACING_CENTRAL, MID_ROWS, stride=SPACING_CENTRAL)


def kernel_call(body, out_shape, operands, scalars, scratch=()):
    in_specs = [pl.BlockSpec(memory_space=pltpu.SMEM)] * scalars + [
        pl.BlockSpec(memory_space=pltpu.VMEM)
    ] * (len(operands) - scalars)
    return pl.pallas_call(
        body,
        out_shape=out_shape,
        in_specs=in_specs,
        out_specs=jax.tree.map(lambda _: pl.BlockSpec(memory_space=pltpu.VMEM), out_shape),
        scratch_shapes=[pltpu.VMEM(dims, jnp.float32) for dims in scratch],
        interpret=INTERPRET,
    )(*operands)


def shaped(*dims):
    return jax.ShapeDtypeStruct(dims, jnp.float32)


def pack_body(count, base, k_ref, v_ref, far_ref, mid_ref, near_ref):
    feature = iota((2 * HEAD, TOKENS), 0)
    live = iota((2 * HEAD, TOKENS), 1) < count[0]
    for j in range(LOCAL_HEADS):
        rows = slice(HEAD * j, HEAD * (j + 1))
        both = jnp.concatenate([k_ref[rows, :], v_ref[rows, :]], axis=0)
        both = jnp.where(live, both, jnp.where(feature == 0, DEAD_MARK, 0.0))
        turned = both.T
        near_ref[TOKENS * j : TOKENS * (j + 1), :] = turned
    for j in range(LOCAL_HEADS):
        head = base[0] + j
        far = near_ref[far_rows(j, head), :]
        mid = near_ref[mid_rows(j, head), :]
        for i in range(far_ref.shape[0]):
            far_ref[i, FAR_ROWS * j : FAR_ROWS * (j + 1), :] = far
        for i in range(mid_ref.shape[0]):
            mid_ref[i, MID_ROWS * j : MID_ROWS * (j + 1), :] = mid


def query_body(count, base, q_ref, w_ref, own_ref, one_ref, two_ref, three_ref, *outs):
    far_ref, mid_ref, near_ref, cot_ref = outs
    columns = own_ref.shape[0]
    heads = cot_ref.shape[0] // columns
    group = base[0] // LOCAL_HEADS
    for k, ref in enumerate((own_ref, one_ref, two_ref, three_ref)):
        at = pl.multiple_of(columns * ((group + heads - k) % heads), columns)
        cot_ref[pl.ds(at, columns), :] = ref[...]
    live = iota((HEAD, TOKENS), 1) < count[0]
    grads = dot3(w_ref[...], cot_ref[...], 1, 0)
    for j in range(LOCAL_HEADS):
        rows = slice(HEAD * j, HEAD * (j + 1))
        both = jnp.concatenate(
            [q_ref[rows, :] * SCALE, jnp.where(live, grads[rows, :], 0.0)], axis=0
        )
        turned = both.T
        near_ref[TOKENS * j : TOKENS * (j + 1), :] = turned
    for j in range(LOCAL_HEADS):
        head = base[0] + j
        far_ref[head_slice(j, FAR_ROWS), :] = near_ref[far_rows(j, head), :]
        mid_ref[head_slice(j, MID_ROWS), :] = near_ref[mid_rows(j, head), :]


def split_queries(turned):
    left = iota(turned.shape, 1) < HEAD
    return jnp.concatenate([jnp.where(left, turned, 0.0), jnp.where(left, 0.0, turned)], axis=0)


def branch_scores(turned, pairs):
    rows = turned.shape[0]
    mark = ((iota((16, 2 * HEAD), 0) == 0) & (iota((16, 2 * HEAD), 1) == 0)).astype(jnp.float32)
    products = dot3(jnp.concatenate([split_queries(turned), mark], axis=0), pairs, 1, 1)
    dead = products[2 * rows : 2 * rows + 1, :] > DEAD_LEVEL
    scores = jnp.where(dead, MASKED_SCORE, products[:rows])
    prob_grads = products[rows : 2 * rows]
    top = jnp.max(scores, axis=1, keepdims=True)
    weights = jnp.exp(scores - top)
    total = jnp.sum(weights, axis=1, keepdims=True)
    pulled = jnp.sum(weights * prob_grads, axis=1, keepdims=True)
    at = iota((rows, 128), 1)
    stats = jnp.where(at == 0, top, jnp.where(at == 1, total, pulled))
    return jnp.concatenate([prob_grads, weights], axis=0), stats


def branch_grads(both, factor, delta):
    rows = both.shape[0] // 2
    probs = both[rows:] * factor
    return jnp.concatenate([probs * (both[:rows] - delta), probs], axis=0)


def query_side(both, pairs):
    rows = both.shape[0] // 2
    sums = dot3(both, pairs, 1, 0)
    left = iota((rows, 2 * HEAD), 1) < HEAD
    return jnp.where(left, sums[:rows], sums[rows:])


def gathered(refs, rows):
    parts = []
    for ref in refs:
        part = ref[:, rows, :]
        parts.append(part.reshape(part.shape[0] * part.shape[1], 128))
    return jnp.concatenate(parts, axis=0)


def head_slice(j, rows):
    return slice(rows * j, rows * (j + 1))


def near_pairs_of(own, other, j):
    rows = head_slice(j, TOKENS)
    return jnp.concatenate([own[rows, :], other[rows, :]], axis=0)


def near_scores_body(q_ref, near_own, near_other, both_ref, stats_ref):
    for j in range(LOCAL_HEADS):
        pairs = near_pairs_of(near_own, near_other, j)
        both_ref[j], stats_ref[j] = branch_scores(q_ref[head_slice(j, TOKENS), :], pairs)


def far_scores_body(q_ref, far_own, far_other, both_ref, stats_ref):
    for j in range(LOCAL_HEADS):
        pairs = gathered((far_own, far_other), head_slice(j, FAR_ROWS))
        both_ref[j], stats_ref[j] = branch_scores(q_ref[head_slice(j, FAR_ROWS), :], pairs)


def attention_body(*refs):
    count, base = refs[:2]
    qm_ref, near_own, near_other, mid_own, mid_other, cot_ref = refs[2:8]
    far_in, far_stats_ref, near_in, near_stats_ref = refs[8:12]
    far_refs = refs[12:14]
    dq_ref, attended_ref, weight_ref, far_both, mid_both, near_both = refs[14:20]
    far_put, mid_put, back_ref, side_ref = refs[20:]
    each = range(LOCAL_HEADS)
    lanes = iota((TOKENS, 128), 1)
    filler = jnp.where(lanes == 0, MASKED_SCORE, 0.0)
    mid_pairs = [gathered((mid_own, mid_other), head_slice(j, MID_ROWS)) for j in each]
    for j in each:
        far_put[head_slice(j, TOKENS), :] = filler
        mid_put[head_slice(j, TOKENS), :] = filler
    starts = [branch_scores(qm_ref[head_slice(j, MID_ROWS), :], mid_pairs[j]) for j in each]
    for j in each:
        far_put[far_rows(j, base[0] + j), :] = far_stats_ref[j]
        mid_put[mid_rows(j, base[0] + j), :] = starts[j][1]
    factors = []
    for j in each:
        far_stats = far_put[head_slice(j, TOKENS), :]
        mid_stats = mid_put[head_slice(j, TOKENS), :]
        near_stats = near_stats_ref[j]
        far_top, mid_top, near_top = far_stats[:, 0:1], mid_stats[:, 0:1], near_stats[:, 0:1]
        top = jnp.maximum(near_top, jnp.maximum(mid_top, far_top))
        far_factor = jnp.exp(far_top - top)
        mid_factor = jnp.exp(mid_top - top)
        near_factor = jnp.exp(near_top - top)
        sums = near_factor * near_stats + mid_factor * mid_stats + far_factor * far_stats
        total = sums[:, 1:2]
        delta = sums[:, 2:3] / total
        near_factor = near_factor / total
        back_ref[head_slice(j, TOKENS), :] = jnp.where(
            lanes == 0, far_factor / total, jnp.where(lanes == 1, mid_factor / total, delta)
        )
        factors.append((near_factor, delta))
    for j in each:
        far_back = back_ref[far_rows(j, base[0] + j), :]
        mid_back = back_ref[mid_rows(j, base[0] + j), :]
        near_both[j] = branch_grads(near_in[j], *factors[j])
        mid_both[j] = branch_grads(starts[j][0], mid_back[:, 1:2], mid_back[:, 2:3])
        far_both[j] = branch_grads(far_in[j], far_back[:, 0:1], far_back[:, 2:3])
    for j in each:
        side_ref[head_slice(j, TOKENS), :] = query_side(
            near_both[j], near_pairs_of(near_own, near_other, j)
        )
    mid_sides = [query_side(mid_both[j], mid_pairs[j]) for j in each]
    far_sides = [query_side(far_both[j], gathered(far_refs, head_slice(j, FAR_ROWS))) for j in each]
    for j in each:
        at = mid_rows(j, base[0] + j)
        side_ref[at, :] = side_ref[at, :] + mid_sides[j]
    for j in each:
        at = far_rows(j, base[0] + j)
        side_ref[at, :] = side_ref[at, :] + far_sides[j]
    live = iota((HEAD, TOKENS), 1) < count[0]
    for j in each:
        turned = side_ref[head_slice(j, TOKENS), :].T
        dq_ref[head_slice(j, HEAD), :] = turned[:HEAD] * SCALE
        attended_ref[head_slice(j, HEAD), :] = jnp.where(live, turned[HEAD:], 0.0)
    columns = attended_ref.shape[0]
    weight = dot3(attended_ref[...], cot_ref[...], 1, 1)
    for b in range(weight.shape[1] // 128):
        weight_ref[columns * b : columns * (b + 1), :] = weight[:, 128 * b : 128 * b + 128]


def terms_body(base, attended_ref, w_ref, *refs):
    term_refs, terms_ref = refs[:4], refs[4]
    terms_ref[...] = dot3(w_ref[...], attended_ref[...], 0, 0)
    columns = term_refs[0].shape[0]
    heads = terms_ref.shape[0] // columns
    group = base[0] // LOCAL_HEADS
    for k, ref in enumerate(term_refs):
        at = pl.multiple_of(columns * ((group + k) % heads), columns)
        ref[...] = terms_ref[pl.ds(at, columns), :]


def wide_keys(both, turned, refs, j):
    sums = outer3(both, split_queries(turned))
    rows = turned.shape[0]
    half = sums.shape[0] // 2
    for i, ref in enumerate(refs):
        ref[:, head_slice(j, rows), :] = sums[half * i : half * (i + 1)].reshape(
            half // rows, rows, 128
        )


def keys_body(far_both, mid_both, near_both, qf_ref, qm_ref, qn_ref, *outs):
    for j in range(LOCAL_HEADS):
        wide_keys(mid_both[j], qm_ref[head_slice(j, MID_ROWS), :], outs[2:4], j)
        wide_keys(far_both[j], qf_ref[head_slice(j, FAR_ROWS), :], outs[:2], j)
        sums = dot3(near_both[j], split_queries(qn_ref[head_slice(j, TOKENS), :]), 0, 0)
        for i, ref in enumerate(outs[4:]):
            ref[head_slice(j, TOKENS), :] = sums[TOKENS * i : TOKENS * (i + 1)]


def finish_body(base, far_ref, mid_ref, near_ref, other_ref, dk_ref, dv_ref, sum_ref):
    far_sum = far_ref[0, :FAR_BLOCK, :]
    for i in range(1, far_ref.shape[0]):
        far_sum = far_sum + far_ref[i, :FAR_BLOCK, :]
    mid_sum = mid_ref[0, :MID_BLOCK, :]
    for i in range(1, mid_ref.shape[0]):
        mid_sum = mid_sum + mid_ref[i, :MID_BLOCK, :]
    sum_ref[...] = near_ref[...] + other_ref[...]
    for j in range(LOCAL_HEADS):
        at = mid_rows(j, base[0] + j)
        sum_ref[at, :] = sum_ref[at, :] + mid_sum[head_slice(j, MID_ROWS)]
    for j in range(LOCAL_HEADS):
        at = far_rows(j, base[0] + j)
        sum_ref[at, :] = sum_ref[at, :] + far_sum[head_slice(j, FAR_ROWS)]
    for j in range(LOCAL_HEADS):
        turned = sum_ref[head_slice(j, TOKENS), :].T
        dk_ref[head_slice(j, HEAD), :] = turned[:HEAD]
        dv_ref[head_slice(j, HEAD), :] = turned[HEAD:]


def exchange(pieces, axis):
    return lax.all_to_all(pieces, axis, 0, 0, tiled=True)


def to_all(piece, axis):
    return exchange(jnp.broadcast_to(piece, (lax.axis_size(axis), *piece.shape)), axis)


def shifted(x, axis, apart):
    size = lax.axis_size(axis)
    return lax.ppermute(x, axis, [(i, (i + apart) % size) for i in range(size)])


def on_device(queries, keys, values, counts, out_weight, cotangent):
    ny, nz, nzh, nzl = (lax.axis_size(axis) for axis in ("y", Z, "zh", "zl"))
    heads = lax.axis_size("h")
    columns, tokens = queries.shape
    base = (lax.axis_index("h") * LOCAL_HEADS).astype(jnp.int32).reshape(1)

    cots = [cotangent] + [shifted(cotangent, "h", k % heads) for k in range(1, 4)]
    far_out, mid_out, near_own = kernel_call(
        pack_body,
        (shaped(nz, FAR_BLOCK, 128), shaped(nzl, MID_BLOCK, 128), shaped(NEAR_BLOCK, 128)),
        (counts, base, keys, values),
        2,
    )
    near_other = shifted(near_own, "c", 1)
    far_line = exchange(far_out, Z)
    query_far, query_mid, query_near, full_cot = kernel_call(
        query_body,
        (
            shaped(FAR_BLOCK, 128),
            shaped(MID_BLOCK, 128),
            shaped(NEAR_BLOCK, 128),
            shaped(heads * columns, tokens),
        ),
        (counts, base, queries, out_weight, *cots),
        2,
    )
    near_both, near_stats = kernel_call(
        near_scores_body,
        (shaped(LOCAL_HEADS, 2 * TOKENS, 2 * TOKENS), shaped(LOCAL_HEADS, TOKENS, 128)),
        (query_near, near_own, near_other),
        0,
    )
    mid_own = exchange(mid_out, "zl")
    far_own = jnp.concatenate(
        [far_line] + [shifted(far_line, "y", k) for k in range(1, ny)], axis=0
    )
    far_other = shifted(far_own, "c", 1)
    far_keys = 2 * ny * nz * FAR_ROWS
    far_both, far_stats = kernel_call(
        far_scores_body,
        (shaped(LOCAL_HEADS, 2 * FAR_ROWS, far_keys), shaped(LOCAL_HEADS, FAR_ROWS, 128)),
        (query_far, far_own, far_other),
        0,
    )
    mid_other = shifted(mid_own, "c", 1)
    mid_keys = 2 * nzl * MID_ROWS
    query_grad, attended, weight, far_both, mid_both, near_both = kernel_call(
        attention_body,
        (
            shaped(columns, tokens),
            shaped(columns, tokens),
            shaped(out_weight.size // 128, 128),
            shaped(LOCAL_HEADS, 2 * FAR_ROWS, far_keys),
            shaped(LOCAL_HEADS, 2 * MID_ROWS, mid_keys),
            shaped(LOCAL_HEADS, 2 * TOKENS, 2 * TOKENS),
        ),
        (
            counts,
            base,
            query_mid,
            near_own,
            near_other,
            mid_own,
            mid_other,
            full_cot,
            far_both,
            far_stats,
            near_both,
            near_stats,
            far_own,
            far_other,
        ),
        2,
        ((NEAR_BLOCK, 128),) * 4,
    )
    planes = 2 * ny
    weight_parts = exchange(weight.reshape(planes, -1, 128), ("y", "c"))
    far_keep, far_send, mid_keep, mid_send, near_keep, near_send = kernel_call(
        keys_body,
        (shaped(ny * nz, FAR_BLOCK, 128),) * 2
        + (shaped(nzl, MID_BLOCK, 128),) * 2
        + (shaped(NEAR_BLOCK, 128),) * 2,
        (far_both, mid_both, near_both, query_far, query_mid, query_near),
        0,
    )
    mid_got = shifted(mid_send, "c", 1)
    weight_line = jnp.sum(weight_parts, axis=0).reshape(nzl, -1, 128)
    mid_sums = exchange(jnp.concatenate([mid_keep + mid_got, weight_line], axis=1), "zl")
    far_got = shifted(far_send, "c", 1)
    near_got = shifted(near_send, "c", 1)
    pieces = [far_keep[nz * k : nz * (k + 1)] + far_got[nz * k : nz * (k + 1)] for k in range(ny)]
    pieces = pieces[:1] + [shifted(pieces[k], "y", -k) for k in range(1, ny)]
    far_total = sum(pieces[1:], pieces[0])
    weight_own = jnp.sum(mid_sums[:, MID_BLOCK:], axis=0)
    depth = weight_own.shape[0]
    parts = exchange(
        jnp.concatenate(
            [far_total, jnp.broadcast_to(weight_own, (nz, depth, 128))], axis=1
        ),
        Z,
    )
    terms = kernel_call(
        terms_body,
        (shaped(columns, tokens),) * 4,
        (base, attended, out_weight),
        1,
        ((heads * columns, tokens),),
    )
    got = [terms[0]] + [shifted(terms[k], "h", k % heads) for k in range(1, 4)]
    output = sum(got[1:], got[0])
    weight_whole = jnp.sum(parts[:, FAR_BLOCK:].reshape(nzh, nzl, depth, 128), axis=0)
    weight_rows = to_all(weight_whole.reshape(nzl * depth, 128), ("y", "c"))
    weight_grad = (
        weight_rows.reshape(out_weight.shape[1] // 128, out_weight.shape[0], 128)
        .swapaxes(0, 1)
        .reshape(out_weight.shape)
    )
    key_grad, value_grad = kernel_call(
        finish_body,
        (shaped(columns, tokens), shaped(columns, tokens)),
        (base, parts, mid_sums, near_keep, near_got),
        1,
        ((NEAR_BLOCK, 128),),
    )
    return output, query_grad, key_grad, value_grad, weight_grad


def solution(mesh):
    split = Mesh(
        mesh.devices.reshape(4, 2, 8, 2, mesh.shape["head"]), ("y", "zh", "zl", "c", "h")
    )
    return on_mesh(split)


def on_mesh(split):
    in_specs = (
        P("h", SEQ),
        P("h", SEQ),
        P("h", SEQ),
        P(SEQ),
        P("h", None),
        P("h", SEQ),
    )
    out_specs = (P("h", SEQ), P("h", SEQ), P("h", SEQ), P("h", SEQ), P("h", None))
    return jax.shard_map(
        on_device, mesh=split, in_specs=in_specs, out_specs=out_specs, check_vma=False
    )
```

```python
import jax
import jax.numpy as jnp
from jax import lax
from jax.experimental import pallas as pl
from jax.experimental.pallas import tpu as pltpu
from jax.sharding import Mesh
from jax.sharding import PartitionSpec as P

HEAD = 64
LOCAL_HEADS = 3
TOKENS = 128
SPACING_CENTRAL = 4
SPACING_WIDE = 16
MID_ROWS = TOKENS // SPACING_CENTRAL
FAR_ROWS = TOKENS // SPACING_WIDE
FAR_BLOCK = LOCAL_HEADS * FAR_ROWS
MID_BLOCK = LOCAL_HEADS * MID_ROWS
NEAR_BLOCK = LOCAL_HEADS * TOKENS
SCALE = HEAD ** (-0.5)
MASKED_SCORE = -1e30
DEAD_MARK = 1e6
DEAD_LEVEL = 1e5
INTERPRET = False
TO_HBM = ("attention",)
SEQ = ("y", "zh", "zl", "c")
Z = ("zh", "zl")


def halves(x):
    high = x.astype(jnp.bfloat16)
    return high, (x - high.astype(jnp.float32)).astype(jnp.bfloat16)


def product(a, b, ca, cb):
    return lax.dot_general(
        a, b, (((ca,), (cb,)), ((), ())), preferred_element_type=jnp.float32
    )


def dot3(a, b, ca, cb):
    a_high, a_low = halves(a)
    b_high, b_low = halves(b)
    if ca == 1:
        rows = a.shape[0]
        both = product(jnp.concatenate([a_high, a_low], axis=0), b_high, ca, cb)
        return both[rows:] + product(a_high, b_low, ca, cb) + both[:rows]
    return product(a_low, b_high, ca, cb) + product(a_high, b_low, ca, cb) + product(a_high, b_high, ca, cb)


def outer3(a, b):
    a_high, a_low = halves(a)
    b_high, b_low = halves(b)
    return product(
        jnp.concatenate([a_low, a_high, a_high], axis=0),
        jnp.concatenate([b_high, b_low, b_high], axis=0),
        0,
        0,
    )


def iota(shape, dim):
    return lax.broadcasted_iota(jnp.int32, shape, dim)


def far_rows(j, head):
    return pl.ds(TOKENS * j + head % SPACING_WIDE, FAR_ROWS, stride=SPACING_WIDE)


def mid_rows(j, head):
    return pl.ds(TOKENS * j + head % SPACING_CENTRAL, MID_ROWS, stride=SPACING_CENTRAL)


def kernel_call(body, out_shape, operands, scalars, name, scratch=()):
    space = pl.BlockSpec(memory_space=pltpu.VMEM)
    in_specs = [pl.BlockSpec(memory_space=pltpu.SMEM)] * scalars + [space] * (
        len(operands) - scalars
    )
    out_specs = jax.tree.map(lambda _: space, out_shape)
    if not INTERPRET and name in TO_HBM:
        out_shape = jax.tree.map(lambda x: pltpu.HBM(x.shape, x.dtype), out_shape)
    return pl.pallas_call(
        body,
        out_shape=out_shape,
        in_specs=in_specs,
        out_specs=out_specs,
        scratch_shapes=[pltpu.VMEM(dims, jnp.float32) for dims in scratch],
        compiler_params=pltpu.CompilerParams(vmem_limit_bytes=16 << 20),
        interpret=INTERPRET,
    )(*operands)


def shaped(*dims):
    return jax.ShapeDtypeStruct(dims, jnp.float32)


def pack_body(count, base, k_ref, v_ref, far_ref, mid_ref, near_ref):
    feature = iota((2 * HEAD, TOKENS), 0)
    live = iota((2 * HEAD, TOKENS), 1) < count[0]
    for j in range(LOCAL_HEADS):
        rows = slice(HEAD * j, HEAD * (j + 1))
        both = jnp.concatenate([k_ref[rows, :], v_ref[rows, :]], axis=0)
        both = jnp.where(live, both, jnp.where(feature == 0, DEAD_MARK, 0.0))
        turned = both.T
        near_ref[TOKENS * j : TOKENS * (j + 1), :] = turned
    for j in range(LOCAL_HEADS):
        head = base[0] + j
        far = near_ref[far_rows(j, head), :]
        mid = near_ref[mid_rows(j, head), :]
        for i in range(far_ref.shape[0]):
            far_ref[i, FAR_ROWS * j : FAR_ROWS * (j + 1), :] = far
        for i in range(mid_ref.shape[0]):
            mid_ref[i, MID_ROWS * j : MID_ROWS * (j + 1), :] = mid


def query_body(count, base, q_ref, w_ref, own_ref, one_ref, two_ref, three_ref, *outs):
    out_ref, cot_ref = outs
    columns = own_ref.shape[0]
    heads = cot_ref.shape[0] // columns
    group = base[0] // LOCAL_HEADS
    for k, ref in enumerate((own_ref, one_ref, two_ref, three_ref)):
        at = pl.multiple_of(columns * ((group + heads - k) % heads), columns)
        cot_ref[pl.ds(at, columns), :] = ref[...]
    live = iota((HEAD, TOKENS), 1) < count[0]
    grads = dot3(w_ref[...], cot_ref[...], 1, 0)
    for j in range(LOCAL_HEADS):
        rows = slice(HEAD * j, HEAD * (j + 1))
        both = jnp.concatenate(
            [q_ref[rows, :] * SCALE, jnp.where(live, grads[rows, :], 0.0)], axis=0
        )
        turned = both.T
        out_ref[head_slice(j, TOKENS), :] = turned
    for j in range(LOCAL_HEADS):
        head = base[0] + j
        far, mid = out_ref[far_rows(j, head), :], out_ref[mid_rows(j, head), :]
        out_ref[NEAR_BLOCK + MID_ROWS * j : NEAR_BLOCK + MID_ROWS * (j + 1), :] = mid
        at = NEAR_BLOCK + MID_BLOCK + FAR_ROWS * j
        out_ref[at : at + FAR_ROWS, :] = far


def split_queries(turned):
    left = iota(turned.shape, 1) < HEAD
    return jnp.concatenate([jnp.where(left, turned, 0.0), jnp.where(left, 0.0, turned)], axis=0)


def branch_scores(turned, pairs):
    rows = turned.shape[0]
    mark = ((iota((16, 2 * HEAD), 0) == 0) & (iota((16, 2 * HEAD), 1) == 0)).astype(jnp.float32)
    products = dot3(jnp.concatenate([split_queries(turned), mark], axis=0), pairs, 1, 1)
    dead = products[2 * rows : 2 * rows + 1, :] > DEAD_LEVEL
    scores = jnp.where(dead, MASKED_SCORE, products[:rows])
    prob_grads = products[rows : 2 * rows]
    top = jnp.max(scores, axis=1, keepdims=True)
    weights = jnp.exp(scores - top)
    total = jnp.sum(weights, axis=1, keepdims=True)
    pulled = jnp.sum(weights * prob_grads, axis=1, keepdims=True)
    at = iota((rows, 128), 1)
    stats = jnp.where(at == 0, top, jnp.where(at == 1, total, pulled))
    return jnp.concatenate([prob_grads, weights], axis=0), stats


def branch_grads(both, factor, delta):
    rows = both.shape[0] // 2
    probs = both[rows:] * factor
    return jnp.concatenate([probs * (both[:rows] - delta), probs], axis=0)


def query_side(both, pairs):
    rows = both.shape[0] // 2
    sums = dot3(both, pairs, 1, 0)
    left = iota((rows, 2 * HEAD), 1) < HEAD
    return jnp.where(left, sums[:rows], sums[rows:])


def gathered(refs, rows):
    parts = []
    for ref in refs:
        part = ref[:, rows, :]
        parts.append(part.reshape(part.shape[0] * part.shape[1], 128))
    return jnp.concatenate(parts, axis=0)


def head_slice(j, rows):
    return slice(rows * j, rows * (j + 1))


def near_pairs_of(own, other, j):
    rows = head_slice(j, TOKENS)
    return jnp.concatenate([own[rows, :], other[rows, :]], axis=0)


def wide_keys(both, turned, refs, j):
    sums = outer3(both, split_queries(turned))
    rows = turned.shape[0]
    half = sums.shape[0] // 2
    for i, ref in enumerate(refs):
        ref[:, head_slice(j, rows), :] = sums[half * i : half * (i + 1)].reshape(
            half // rows, rows, 128
        )


def attention_body(*refs):
    count, base = refs[:2]
    q_ref, near_own, near_other, mid_own, mid_other, cot_ref = refs[2:8]
    far_refs = refs[8:10]
    dq_ref, attended_ref, weight_ref = refs[10:13]
    far_outs, mid_outs, near_outs = refs[13:15], refs[15:17], refs[17:19]
    far_put, mid_put, back_ref, side_ref = refs[19:]
    each = range(LOCAL_HEADS)
    lanes = iota((TOKENS, 128), 1)
    filler = jnp.where(lanes == 0, MASKED_SCORE, 0.0)
    mid_pairs = [gathered((mid_own, mid_other), head_slice(j, MID_ROWS)) for j in each]
    for j in each:
        far_put[head_slice(j, TOKENS), :] = filler
        mid_put[head_slice(j, TOKENS), :] = filler
    mid_at, far_at = NEAR_BLOCK, NEAR_BLOCK + MID_BLOCK
    near_q = [q_ref[head_slice(j, TOKENS), :] for j in each]
    mid_q = [q_ref[mid_at + MID_ROWS * j : mid_at + MID_ROWS * (j + 1), :] for j in each]
    far_q = [q_ref[far_at + FAR_ROWS * j : far_at + FAR_ROWS * (j + 1), :] for j in each]
    near_pairs = [near_pairs_of(near_own, near_other, j) for j in each]
    far_pairs = [gathered(far_refs, head_slice(j, FAR_ROWS)) for j in each]
    near_starts = [branch_scores(near_q[j], near_pairs[j]) for j in each]
    far_starts = [branch_scores(far_q[j], far_pairs[j]) for j in each]
    starts = [branch_scores(mid_q[j], mid_pairs[j]) for j in each]
    for j in each:
        far_put[far_rows(j, base[0] + j), :] = far_starts[j][1]
        mid_put[mid_rows(j, base[0] + j), :] = starts[j][1]
    factors = []
    far_both, mid_both, near_both = [None] * 3, [None] * 3, [None] * 3
    for j in each:
        far_stats = far_put[head_slice(j, TOKENS), :]
        mid_stats = mid_put[head_slice(j, TOKENS), :]
        near_stats = near_starts[j][1]
        far_top, mid_top, near_top = far_stats[:, 0:1], mid_stats[:, 0:1], near_stats[:, 0:1]
        top = jnp.maximum(near_top, jnp.maximum(mid_top, far_top))
        far_factor = jnp.exp(far_top - top)
        mid_factor = jnp.exp(mid_top - top)
        near_factor = jnp.exp(near_top - top)
        sums = near_factor * near_stats + mid_factor * mid_stats + far_factor * far_stats
        total = sums[:, 1:2]
        delta = sums[:, 2:3] / total
        near_factor = near_factor / total
        back_ref[head_slice(j, TOKENS), :] = jnp.where(
            lanes == 0, far_factor / total, jnp.where(lanes == 1, mid_factor / total, delta)
        )
        factors.append((near_factor, delta))
    for j in each:
        far_back = back_ref[far_rows(j, base[0] + j), :]
        mid_back = back_ref[mid_rows(j, base[0] + j), :]
        near_both[j] = branch_grads(near_starts[j][0], *factors[j])
        mid_both[j] = branch_grads(starts[j][0], mid_back[:, 1:2], mid_back[:, 2:3])
        far_both[j] = branch_grads(far_starts[j][0], far_back[:, 0:1], far_back[:, 2:3])
    for j in each:
        side_ref[head_slice(j, TOKENS), :] = query_side(
            near_both[j], near_pairs[j]
        )
    mid_sides = [query_side(mid_both[j], mid_pairs[j]) for j in each]
    far_sides = [query_side(far_both[j], far_pairs[j]) for j in each]
    for j in each:
        at = mid_rows(j, base[0] + j)
        side_ref[at, :] = side_ref[at, :] + mid_sides[j]
    for j in each:
        at = far_rows(j, base[0] + j)
        side_ref[at, :] = side_ref[at, :] + far_sides[j]
    live = iota((HEAD, TOKENS), 1) < count[0]
    for j in each:
        turned = side_ref[head_slice(j, TOKENS), :].T
        dq_ref[head_slice(j, HEAD), :] = turned[:HEAD] * SCALE
        attended_ref[head_slice(j, HEAD), :] = jnp.where(live, turned[HEAD:], 0.0)
    columns = attended_ref.shape[0]
    weight = dot3(attended_ref[...], cot_ref[...], 1, 1)
    for b in range(weight.shape[1] // 128):
        weight_ref[columns * b : columns * (b + 1), :] = weight[:, 128 * b : 128 * b + 128]
    for j in each:
        wide_keys(mid_both[j], mid_q[j], mid_outs, j)
        wide_keys(far_both[j], far_q[j], far_outs, j)
        sums = dot3(near_both[j], split_queries(near_q[j]), 0, 0)
        for i, ref in enumerate(near_outs):
            ref[head_slice(j, TOKENS), :] = sums[TOKENS * i : TOKENS * (i + 1)]


def terms_body(base, attended_ref, w_ref, *refs):
    term_refs, terms_ref = refs[:4], refs[4]
    terms_ref[...] = dot3(w_ref[...], attended_ref[...], 0, 0)
    columns = term_refs[0].shape[0]
    heads = terms_ref.shape[0] // columns
    group = base[0] // LOCAL_HEADS
    for k, ref in enumerate(term_refs):
        at = pl.multiple_of(columns * ((group + k) % heads), columns)
        ref[...] = terms_ref[pl.ds(at, columns), :]


def finish_body(base, far_ref, mid_ref, near_ref, other_ref, dk_ref, dv_ref, sum_ref):
    far_sum = far_ref[0, :FAR_BLOCK, :]
    for i in range(1, far_ref.shape[0]):
        far_sum = far_sum + far_ref[i, :FAR_BLOCK, :]
    mid_sum = mid_ref[0, :MID_BLOCK, :]
    for i in range(1, mid_ref.shape[0]):
        mid_sum = mid_sum + mid_ref[i, :MID_BLOCK, :]
    sum_ref[...] = near_ref[...] + other_ref[...]
    for j in range(LOCAL_HEADS):
        at = mid_rows(j, base[0] + j)
        sum_ref[at, :] = sum_ref[at, :] + mid_sum[head_slice(j, MID_ROWS)]
    for j in range(LOCAL_HEADS):
        at = far_rows(j, base[0] + j)
        sum_ref[at, :] = sum_ref[at, :] + far_sum[head_slice(j, FAR_ROWS)]
    for j in range(LOCAL_HEADS):
        turned = sum_ref[head_slice(j, TOKENS), :].T
        dk_ref[head_slice(j, HEAD), :] = turned[:HEAD]
        dv_ref[head_slice(j, HEAD), :] = turned[HEAD:]


def exchange(pieces, axis):
    return lax.all_to_all(pieces, axis, 0, 0, tiled=True)


def to_all(piece, axis):
    return exchange(jnp.broadcast_to(piece, (lax.axis_size(axis), *piece.shape)), axis)


def shifted(x, axis, apart):
    size = lax.axis_size(axis)
    return lax.ppermute(x, axis, [(i, (i + apart) % size) for i in range(size)])


def on_device(queries, keys, values, counts, out_weight, cotangent):
    ny, nz, nzh, nzl = (lax.axis_size(axis) for axis in ("y", Z, "zh", "zl"))
    heads = lax.axis_size("h")
    columns, tokens = queries.shape
    base = (lax.axis_index("h") * LOCAL_HEADS).astype(jnp.int32).reshape(1)

    cots = [cotangent] + [shifted(cotangent, "h", k % heads) for k in range(1, 4)]
    far_out, mid_out, near_own = kernel_call(
        pack_body,
        (shaped(nz, FAR_BLOCK, 128), shaped(nzl, MID_BLOCK, 128), shaped(NEAR_BLOCK, 128)),
        (counts, base, keys, values),
        2,
        "pack",
    )
    near_other = shifted(near_own, "c", 1)
    far_line = exchange(far_out, Z)
    query_rows, full_cot = kernel_call(
        query_body,
        (
            shaped(NEAR_BLOCK + MID_BLOCK + FAR_BLOCK, 128),
            shaped(heads * columns, tokens),
        ),
        (counts, base, queries, out_weight, *cots),
        2,
        "query",
    )
    mid_own = exchange(mid_out, "zl")
    far_lines = [far_line] + [shifted(far_line, "y", k) for k in range(1, ny)]
    far_own = jnp.concatenate(far_lines, axis=0)
    far_other = shifted(far_own, "c", 1)
    mid_other = shifted(mid_own, "c", 1)
    (
        query_grad,
        attended,
        weight,
        far_keep,
        far_send,
        mid_keep,
        mid_send,
        near_keep,
        near_send,
    ) = kernel_call(
        attention_body,
        (
            shaped(columns, tokens),
            shaped(columns, tokens),
            shaped(out_weight.size // 128, 128),
        )
        + (shaped(ny * nz, FAR_BLOCK, 128),) * 2
        + (shaped(nzl, MID_BLOCK, 128),) * 2
        + (shaped(NEAR_BLOCK, 128),) * 2,
        (
            counts,
            base,
            query_rows,
            near_own,
            near_other,
            mid_own,
            mid_other,
            full_cot,
            far_own,
            far_other,
        ),
        2,
        "attention",
        ((NEAR_BLOCK, 128),) * 4,
    )
    planes = 2 * ny
    weight_parts = exchange(weight.reshape(planes, -1, 128), ("y", "c"))
    mid_got = shifted(mid_send, "c", 1)
    weight_line = jnp.sum(weight_parts, axis=0).reshape(nzl, -1, 128)
    mid_total = mid_keep + mid_got
    mid_sums = exchange(jnp.concatenate([mid_total, weight_line], axis=1), "zl")
    far_got = shifted(far_send, "c", 1)
    near_got = shifted(near_send, "c", 1)
    pieces = [far_keep[nz * k : nz * (k + 1)] + far_got[nz * k : nz * (k + 1)] for k in range(ny)]
    pieces = pieces[:1] + [shifted(pieces[k], "y", -k) for k in range(1, ny)]
    far_total = sum(pieces[1:], pieces[0])
    weight_own = jnp.sum(mid_sums[:, MID_BLOCK:], axis=0)
    depth = weight_own.shape[0]
    parts = exchange(
        jnp.concatenate(
            [far_total, jnp.broadcast_to(weight_own, (nz, depth, 128))], axis=1
        ),
        Z,
    )
    terms = kernel_call(
        terms_body,
        (shaped(columns, tokens),) * 4,
        (base, attended, out_weight),
        1,
        "terms",
        ((heads * columns, tokens),),
    )
    got = [terms[0]] + [shifted(terms[k], "h", k % heads) for k in range(1, 4)]
    output = sum(got[1:], got[0])
    weight_whole = jnp.sum(parts[:, FAR_BLOCK:].reshape(nzh, nzl, depth, 128), axis=0)
    weight_rows = to_all(weight_whole.reshape(nzl * depth, 128), ("y", "c"))
    weight_grad = (
        weight_rows.reshape(out_weight.shape[1] // 128, out_weight.shape[0], 128)
        .swapaxes(0, 1)
        .reshape(out_weight.shape)
    )
    key_grad, value_grad = kernel_call(
        finish_body,
        (shaped(columns, tokens), shaped(columns, tokens)),
        (base, parts, mid_sums, near_keep, near_got),
        1,
        "finish",
        ((NEAR_BLOCK, 128),),
    )
    return output, query_grad, key_grad, value_grad, weight_grad


def solution(mesh):
    split = Mesh(
        mesh.devices.reshape(4, 2, 8, 2, mesh.shape["head"]), ("y", "zh", "zl", "c", "h")
    )
    return on_mesh(split)


def on_mesh(split):
    in_specs = (
        P("h", SEQ),
        P("h", SEQ),
        P("h", SEQ),
        P(SEQ),
        P("h", None),
        P("h", SEQ),
    )
    out_specs = (P("h", SEQ), P("h", SEQ), P("h", SEQ), P("h", SEQ), P("h", None))
    return jax.shard_map(
        on_device, mesh=split, in_specs=in_specs, out_specs=out_specs, check_vma=False
    )
```

```python
import jax
import jax.numpy as jnp
from jax import lax
from jax.experimental import pallas as pl
from jax.experimental.pallas import tpu as pltpu
from jax.sharding import Mesh
from jax.sharding import PartitionSpec as P

HEAD = 64
LOCAL_HEADS = 3
TOKENS = 128
SPACING_CENTRAL = 4
SPACING_WIDE = 16
MID_ROWS = TOKENS // SPACING_CENTRAL
FAR_ROWS = TOKENS // SPACING_WIDE
FAR_BLOCK = LOCAL_HEADS * FAR_ROWS
MID_BLOCK = LOCAL_HEADS * MID_ROWS
NEAR_BLOCK = LOCAL_HEADS * TOKENS
SCALE = HEAD ** (-0.5)
MASKED_SCORE = -1e30
DEAD_MARK = 1e6
DEAD_LEVEL = 1e5
INTERPRET = False
TO_HBM = ("attention", "keys")
SEQ = ("y", "zh", "zl", "c")
Z = ("zh", "zl")


def halves(x):
    high = x.astype(jnp.bfloat16)
    return high, (x - high.astype(jnp.float32)).astype(jnp.bfloat16)


def product(a, b, ca, cb):
    return lax.dot_general(
        a, b, (((ca,), (cb,)), ((), ())), preferred_element_type=jnp.float32
    )


def dot3(a, b, ca, cb):
    a_high, a_low = halves(a)
    b_high, b_low = halves(b)
    if ca == 1:
        rows = a.shape[0]
        both = product(jnp.concatenate([a_high, a_low], axis=0), b_high, ca, cb)
        return both[rows:] + product(a_high, b_low, ca, cb) + both[:rows]
    return product(a_low, b_high, ca, cb) + product(a_high, b_low, ca, cb) + product(a_high, b_high, ca, cb)


def outer3(a, b):
    a_high, a_low = halves(a)
    b_high, b_low = halves(b)
    return product(
        jnp.concatenate([a_low, a_high, a_high], axis=0),
        jnp.concatenate([b_high, b_low, b_high], axis=0),
        0,
        0,
    )


def iota(shape, dim):
    return lax.broadcasted_iota(jnp.int32, shape, dim)


def far_rows(j, head):
    return pl.ds(TOKENS * j + head % SPACING_WIDE, FAR_ROWS, stride=SPACING_WIDE)


def mid_rows(j, head):
    return pl.ds(TOKENS * j + head % SPACING_CENTRAL, MID_ROWS, stride=SPACING_CENTRAL)


def kernel_call(body, out_shape, operands, scalars, name, scratch=(), from_hbm=()):
    space = pl.BlockSpec(memory_space=pltpu.VMEM)
    in_specs = [pl.BlockSpec(memory_space=pltpu.SMEM)] * scalars + [space] * (
        len(operands) - scalars
    )
    out_specs = jax.tree.map(lambda _: space, out_shape)
    if not INTERPRET:
        operands = [
            pltpu.with_memory_space_constraint(x, pltpu.HBM) if i in from_hbm else x
            for i, x in enumerate(operands)
        ]
    if not INTERPRET and name in TO_HBM:
        out_shape = jax.tree.map(lambda x: pltpu.HBM(x.shape, x.dtype), out_shape)
    return pl.pallas_call(
        body,
        out_shape=out_shape,
        in_specs=in_specs,
        out_specs=out_specs,
        scratch_shapes=[pltpu.VMEM(dims, jnp.float32) for dims in scratch],
        compiler_params=pltpu.CompilerParams(vmem_limit_bytes=16 << 20),
        interpret=INTERPRET,
    )(*operands)


def shaped(*dims):
    return jax.ShapeDtypeStruct(dims, jnp.float32)


def pack_body(count, base, k_ref, v_ref, far_ref, mid_ref, near_ref):
    feature = iota((2 * HEAD, TOKENS), 0)
    live = iota((2 * HEAD, TOKENS), 1) < count[0]
    for j in range(LOCAL_HEADS):
        rows = slice(HEAD * j, HEAD * (j + 1))
        both = jnp.concatenate([k_ref[rows, :], v_ref[rows, :]], axis=0)
        both = jnp.where(live, both, jnp.where(feature == 0, DEAD_MARK, 0.0))
        turned = both.T
        near_ref[TOKENS * j : TOKENS * (j + 1), :] = turned
    for j in range(LOCAL_HEADS):
        head = base[0] + j
        far = near_ref[far_rows(j, head), :]
        mid = near_ref[mid_rows(j, head), :]
        for i in range(far_ref.shape[0]):
            far_ref[i, FAR_ROWS * j : FAR_ROWS * (j + 1), :] = far
        for i in range(mid_ref.shape[0]):
            mid_ref[i, MID_ROWS * j : MID_ROWS * (j + 1), :] = mid


def query_body(count, base, q_ref, w_ref, own_ref, one_ref, two_ref, three_ref, *outs):
    out_ref, cot_ref = outs
    columns = own_ref.shape[0]
    heads = cot_ref.shape[0] // columns
    group = base[0] // LOCAL_HEADS
    for k, ref in enumerate((own_ref, one_ref, two_ref, three_ref)):
        at = pl.multiple_of(columns * ((group + heads - k) % heads), columns)
        cot_ref[pl.ds(at, columns), :] = ref[...]
    live = iota((HEAD, TOKENS), 1) < count[0]
    grads = dot3(w_ref[...], cot_ref[...], 1, 0)
    for j in range(LOCAL_HEADS):
        rows = slice(HEAD * j, HEAD * (j + 1))
        both = jnp.concatenate(
            [q_ref[rows, :] * SCALE, jnp.where(live, grads[rows, :], 0.0)], axis=0
        )
        turned = both.T
        out_ref[head_slice(j, TOKENS), :] = turned
    for j in range(LOCAL_HEADS):
        head = base[0] + j
        far, mid = out_ref[far_rows(j, head), :], out_ref[mid_rows(j, head), :]
        out_ref[NEAR_BLOCK + MID_ROWS * j : NEAR_BLOCK + MID_ROWS * (j + 1), :] = mid
        at = NEAR_BLOCK + MID_BLOCK + FAR_ROWS * j
        out_ref[at : at + FAR_ROWS, :] = far


def split_queries(turned):
    left = iota(turned.shape, 1) < HEAD
    return jnp.concatenate([jnp.where(left, turned, 0.0), jnp.where(left, 0.0, turned)], axis=0)


def branch_scores(turned, pairs):
    rows = turned.shape[0]
    mark = ((iota((16, 2 * HEAD), 0) == 0) & (iota((16, 2 * HEAD), 1) == 0)).astype(jnp.float32)
    products = dot3(jnp.concatenate([split_queries(turned), mark], axis=0), pairs, 1, 1)
    dead = products[2 * rows : 2 * rows + 1, :] > DEAD_LEVEL
    scores = jnp.where(dead, MASKED_SCORE, products[:rows])
    prob_grads = products[rows : 2 * rows]
    top = jnp.max(scores, axis=1, keepdims=True)
    weights = jnp.exp(scores - top)
    total = jnp.sum(weights, axis=1, keepdims=True)
    pulled = jnp.sum(weights * prob_grads, axis=1, keepdims=True)
    at = iota((rows, 128), 1)
    stats = jnp.where(at == 0, top, jnp.where(at == 1, total, pulled))
    return jnp.concatenate([prob_grads, weights], axis=0), stats


def branch_grads(both, factor, delta):
    rows = both.shape[0] // 2
    probs = both[rows:] * factor
    return jnp.concatenate([probs * (both[:rows] - delta), probs], axis=0)


def query_side(both, pairs):
    rows = both.shape[0] // 2
    sums = dot3(both, pairs, 1, 0)
    left = iota((rows, 2 * HEAD), 1) < HEAD
    return jnp.where(left, sums[:rows], sums[rows:])


def gathered(refs, rows):
    parts = []
    for ref in refs:
        part = ref[:, rows, :]
        parts.append(part.reshape(part.shape[0] * part.shape[1], 128))
    return jnp.concatenate(parts, axis=0)


def head_slice(j, rows):
    return slice(rows * j, rows * (j + 1))


def near_pairs_of(own, other, j):
    rows = head_slice(j, TOKENS)
    return jnp.concatenate([own[rows, :], other[rows, :]], axis=0)


def wide_keys(both, turned, refs, j):
    sums = outer3(both, split_queries(turned))
    rows = turned.shape[0]
    half = sums.shape[0] // 2
    for i, ref in enumerate(refs):
        ref[:, head_slice(j, rows), :] = sums[half * i : half * (i + 1)].reshape(
            half // rows, rows, 128
        )


def attention_body(*refs):
    count, base = refs[:2]
    q_ref, near_own, near_other, mid_own, mid_other, cot_ref = refs[2:8]
    far_refs = refs[8:10]
    dq_ref, attended_ref, weight_ref = refs[10:13]
    far_out, mid_out, near_out = refs[13:16]
    far_put, mid_put, back_ref, side_ref = refs[16:]
    each = range(LOCAL_HEADS)
    lanes = iota((TOKENS, 128), 1)
    filler = jnp.where(lanes == 0, MASKED_SCORE, 0.0)
    mid_pairs = [gathered((mid_own, mid_other), head_slice(j, MID_ROWS)) for j in each]
    for j in each:
        far_put[head_slice(j, TOKENS), :] = filler
        mid_put[head_slice(j, TOKENS), :] = filler
    mid_at, far_at = NEAR_BLOCK, NEAR_BLOCK + MID_BLOCK
    near_q = [q_ref[head_slice(j, TOKENS), :] for j in each]
    mid_q = [q_ref[mid_at + MID_ROWS * j : mid_at + MID_ROWS * (j + 1), :] for j in each]
    far_q = [q_ref[far_at + FAR_ROWS * j : far_at + FAR_ROWS * (j + 1), :] for j in each]
    near_pairs = [near_pairs_of(near_own, near_other, j) for j in each]
    far_pairs = [gathered(far_refs, head_slice(j, FAR_ROWS)) for j in each]
    near_starts = [branch_scores(near_q[j], near_pairs[j]) for j in each]
    far_starts = [branch_scores(far_q[j], far_pairs[j]) for j in each]
    starts = [branch_scores(mid_q[j], mid_pairs[j]) for j in each]
    for j in each:
        far_put[far_rows(j, base[0] + j), :] = far_starts[j][1]
        mid_put[mid_rows(j, base[0] + j), :] = starts[j][1]
    factors = []
    far_both, mid_both, near_both = [None] * 3, [None] * 3, [None] * 3
    for j in each:
        far_stats = far_put[head_slice(j, TOKENS), :]
        mid_stats = mid_put[head_slice(j, TOKENS), :]
        near_stats = near_starts[j][1]
        far_top, mid_top, near_top = far_stats[:, 0:1], mid_stats[:, 0:1], near_stats[:, 0:1]
        top = jnp.maximum(near_top, jnp.maximum(mid_top, far_top))
        far_factor = jnp.exp(far_top - top)
        mid_factor = jnp.exp(mid_top - top)
        near_factor = jnp.exp(near_top - top)
        sums = near_factor * near_stats + mid_factor * mid_stats + far_factor * far_stats
        total = sums[:, 1:2]
        delta = sums[:, 2:3] / total
        near_factor = near_factor / total
        back_ref[head_slice(j, TOKENS), :] = jnp.where(
            lanes == 0, far_factor / total, jnp.where(lanes == 1, mid_factor / total, delta)
        )
        factors.append((near_factor, delta))
    for j in each:
        far_back = back_ref[far_rows(j, base[0] + j), :]
        mid_back = back_ref[mid_rows(j, base[0] + j), :]
        near_both[j] = branch_grads(near_starts[j][0], *factors[j])
        mid_both[j] = branch_grads(starts[j][0], mid_back[:, 1:2], mid_back[:, 2:3])
        far_both[j] = branch_grads(far_starts[j][0], far_back[:, 0:1], far_back[:, 2:3])
    for j in each:
        far_out[j] = far_both[j]
        mid_out[j] = mid_both[j]
        near_out[j] = near_both[j]
    for j in each:
        side_ref[head_slice(j, TOKENS), :] = query_side(
            near_both[j], near_pairs[j]
        )
    mid_sides = [query_side(mid_both[j], mid_pairs[j]) for j in each]
    far_sides = [query_side(far_both[j], far_pairs[j]) for j in each]
    for j in each:
        at = mid_rows(j, base[0] + j)
        side_ref[at, :] = side_ref[at, :] + mid_sides[j]
    for j in each:
        at = far_rows(j, base[0] + j)
        side_ref[at, :] = side_ref[at, :] + far_sides[j]
    live = iota((HEAD, TOKENS), 1) < count[0]
    for j in each:
        turned = side_ref[head_slice(j, TOKENS), :].T
        dq_ref[head_slice(j, HEAD), :] = turned[:HEAD] * SCALE
        attended_ref[head_slice(j, HEAD), :] = jnp.where(live, turned[HEAD:], 0.0)
    columns = attended_ref.shape[0]
    weight = dot3(attended_ref[...], cot_ref[...], 1, 1)
    for b in range(weight.shape[1] // 128):
        weight_ref[columns * b : columns * (b + 1), :] = weight[:, 128 * b : 128 * b + 128]


def keys_body(far_both, mid_both, near_both, q_ref, *outs):
    mid_at, far_at = NEAR_BLOCK, NEAR_BLOCK + MID_BLOCK
    for j in range(LOCAL_HEADS):
        mid_q = q_ref[mid_at + MID_ROWS * j : mid_at + MID_ROWS * (j + 1), :]
        far_q = q_ref[far_at + FAR_ROWS * j : far_at + FAR_ROWS * (j + 1), :]
        wide_keys(mid_both[j], mid_q, outs[2:4], j)
        wide_keys(far_both[j], far_q, outs[:2], j)
        sums = dot3(near_both[j], split_queries(q_ref[head_slice(j, TOKENS), :]), 0, 0)
        for i, ref in enumerate(outs[4:]):
            ref[head_slice(j, TOKENS), :] = sums[TOKENS * i : TOKENS * (i + 1)]


def terms_body(base, attended_ref, w_ref, *refs):
    term_refs, terms_ref = refs[:4], refs[4]
    terms_ref[...] = dot3(w_ref[...], attended_ref[...], 0, 0)
    columns = term_refs[0].shape[0]
    heads = terms_ref.shape[0] // columns
    group = base[0] // LOCAL_HEADS
    for k, ref in enumerate(term_refs):
        at = pl.multiple_of(columns * ((group + k) % heads), columns)
        ref[...] = terms_ref[pl.ds(at, columns), :]


def finish_body(base, far_ref, mid_ref, near_ref, other_ref, dk_ref, dv_ref, sum_ref):
    far_sum = far_ref[0, :FAR_BLOCK, :]
    for i in range(1, far_ref.shape[0]):
        far_sum = far_sum + far_ref[i, :FAR_BLOCK, :]
    mid_sum = mid_ref[0, :MID_BLOCK, :]
    for i in range(1, mid_ref.shape[0]):
        mid_sum = mid_sum + mid_ref[i, :MID_BLOCK, :]
    sum_ref[...] = near_ref[...] + other_ref[...]
    for j in range(LOCAL_HEADS):
        at = mid_rows(j, base[0] + j)
        sum_ref[at, :] = sum_ref[at, :] + mid_sum[head_slice(j, MID_ROWS)]
    for j in range(LOCAL_HEADS):
        at = far_rows(j, base[0] + j)
        sum_ref[at, :] = sum_ref[at, :] + far_sum[head_slice(j, FAR_ROWS)]
    for j in range(LOCAL_HEADS):
        turned = sum_ref[head_slice(j, TOKENS), :].T
        dk_ref[head_slice(j, HEAD), :] = turned[:HEAD]
        dv_ref[head_slice(j, HEAD), :] = turned[HEAD:]


def exchange(pieces, axis):
    return lax.all_to_all(pieces, axis, 0, 0, tiled=True)


def to_all(piece, axis):
    return exchange(jnp.broadcast_to(piece, (lax.axis_size(axis), *piece.shape)), axis)


def shifted(x, axis, apart):
    size = lax.axis_size(axis)
    return lax.ppermute(x, axis, [(i, (i + apart) % size) for i in range(size)])


def on_device(queries, keys, values, counts, out_weight, cotangent):
    ny, nz, nzh, nzl = (lax.axis_size(axis) for axis in ("y", Z, "zh", "zl"))
    heads = lax.axis_size("h")
    columns, tokens = queries.shape
    base = (lax.axis_index("h") * LOCAL_HEADS).astype(jnp.int32).reshape(1)

    cots = [cotangent] + [shifted(cotangent, "h", k % heads) for k in range(1, 4)]
    far_out, mid_out, near_own = kernel_call(
        pack_body,
        (shaped(nz, FAR_BLOCK, 128), shaped(nzl, MID_BLOCK, 128), shaped(NEAR_BLOCK, 128)),
        (counts, base, keys, values),
        2,
        "pack",
        (),
        (2, 3),
    )
    near_other = shifted(near_own, "c", 1)
    far_line = exchange(far_out, Z)
    query_rows, full_cot = kernel_call(
        query_body,
        (
            shaped(NEAR_BLOCK + MID_BLOCK + FAR_BLOCK, 128),
            shaped(heads * columns, tokens),
        ),
        (counts, base, queries, out_weight, *cots),
        2,
        "query",
        (),
        (2, 4),
    )
    mid_own = exchange(mid_out, "zl")
    far_lines = [far_line] + [shifted(far_line, "y", k) for k in range(1, ny)]
    far_own = jnp.concatenate(far_lines, axis=0)
    far_other = shifted(far_own, "c", 1)
    mid_other = shifted(mid_own, "c", 1)
    far_keys, mid_keys = 2 * ny * nz * FAR_ROWS, 2 * nzl * MID_ROWS
    query_grad, attended, weight, far_both, mid_both, near_both = kernel_call(
        attention_body,
        (
            shaped(columns, tokens),
            shaped(columns, tokens),
            shaped(out_weight.size // 128, 128),
            shaped(LOCAL_HEADS, 2 * FAR_ROWS, far_keys),
            shaped(LOCAL_HEADS, 2 * MID_ROWS, mid_keys),
            shaped(LOCAL_HEADS, 2 * TOKENS, 2 * TOKENS),
        ),
        (
            counts,
            base,
            query_rows,
            near_own,
            near_other,
            mid_own,
            mid_other,
            full_cot,
            far_own,
            far_other,
        ),
        2,
        "attention",
        ((NEAR_BLOCK, 128),) * 4,
    )
    planes = 2 * ny
    weight_parts = exchange(weight.reshape(planes, -1, 128), ("y", "c"))
    far_keep, far_send, mid_keep, mid_send, near_keep, near_send = kernel_call(
        keys_body,
        (shaped(ny * nz, FAR_BLOCK, 128),) * 2
        + (shaped(nzl, MID_BLOCK, 128),) * 2
        + (shaped(NEAR_BLOCK, 128),) * 2,
        (far_both, mid_both, near_both, query_rows),
        0,
        "keys",
        (),
        (0, 1, 2),
    )
    mid_got = shifted(mid_send, "c", 1)
    weight_line = jnp.sum(weight_parts, axis=0).reshape(nzl, -1, 128)
    mid_total = mid_keep + mid_got
    mid_sums = exchange(jnp.concatenate([mid_total, weight_line], axis=1), "zl")
    far_got = shifted(far_send, "c", 1)
    near_got = shifted(near_send, "c", 1)
    pieces = [far_keep[nz * k : nz * (k + 1)] + far_got[nz * k : nz * (k + 1)] for k in range(ny)]
    pieces = pieces[:1] + [shifted(pieces[k], "y", -k) for k in range(1, ny)]
    far_total = sum(pieces[1:], pieces[0])
    weight_own = jnp.sum(mid_sums[:, MID_BLOCK:], axis=0)
    depth = weight_own.shape[0]
    parts = exchange(
        jnp.concatenate(
            [far_total, jnp.broadcast_to(weight_own, (nz, depth, 128))], axis=1
        ),
        Z,
    )
    terms = kernel_call(
        terms_body,
        (shaped(columns, tokens),) * 4,
        (base, attended, out_weight),
        1,
        "terms",
        ((heads * columns, tokens),),
    )
    got = [terms[0]] + [shifted(terms[k], "h", k % heads) for k in range(1, 4)]
    output = sum(got[1:], got[0])
    weight_whole = jnp.sum(parts[:, FAR_BLOCK:].reshape(nzh, nzl, depth, 128), axis=0)
    weight_rows = to_all(weight_whole.reshape(nzl * depth, 128), ("y", "c"))
    weight_grad = (
        weight_rows.reshape(out_weight.shape[1] // 128, out_weight.shape[0], 128)
        .swapaxes(0, 1)
        .reshape(out_weight.shape)
    )
    key_grad, value_grad = kernel_call(
        finish_body,
        (shaped(columns, tokens), shaped(columns, tokens)),
        (base, parts, mid_sums, near_keep, near_got),
        1,
        "finish",
        ((NEAR_BLOCK, 128),),
    )
    return output, query_grad, key_grad, value_grad, weight_grad


def solution(mesh):
    split = Mesh(
        mesh.devices.reshape(4, 2, 8, 2, mesh.shape["head"]), ("y", "zh", "zl", "c", "h")
    )
    return on_mesh(split)


def on_mesh(split):
    in_specs = (
        P("h", SEQ),
        P("h", SEQ),
        P("h", SEQ),
        P(SEQ),
        P("h", None),
        P("h", SEQ),
    )
    out_specs = (P("h", SEQ), P("h", SEQ), P("h", SEQ), P("h", SEQ), P("h", None))
    return jax.shard_map(
        on_device, mesh=split, in_specs=in_specs, out_specs=out_specs, check_vma=False
    )
```

```python
import jax
import jax.numpy as jnp
from jax import lax
from jax.experimental import pallas as pl
from jax.experimental.pallas import tpu as pltpu
from jax.sharding import Mesh
from jax.sharding import PartitionSpec as P

HEAD = 64
LOCAL_HEADS = 3
TOKENS = 128
SPACING_CENTRAL = 4
SPACING_WIDE = 16
MID_ROWS = TOKENS // SPACING_CENTRAL
FAR_ROWS = TOKENS // SPACING_WIDE
FAR_BLOCK = LOCAL_HEADS * FAR_ROWS
MID_BLOCK = LOCAL_HEADS * MID_ROWS
NEAR_BLOCK = LOCAL_HEADS * TOKENS
SCALE = HEAD ** (-0.5)
MASKED_SCORE = -1e30
DEAD_MARK = 1e6
DEAD_LEVEL = 1e5
INTERPRET = False
TO_HBM = ("attention", "keys")
SEQ = ("y", "zh", "zl", "c")
Z = ("zh", "zl")


def halves(x):
    high = x.astype(jnp.bfloat16)
    return high, (x - high.astype(jnp.float32)).astype(jnp.bfloat16)


def product(a, b, ca, cb):
    return lax.dot_general(
        a, b, (((ca,), (cb,)), ((), ())), preferred_element_type=jnp.float32
    )


def dot3(a, b, ca, cb):
    a_high, a_low = halves(a)
    b_high, b_low = halves(b)
    if ca == 1:
        rows = a.shape[0]
        both = product(jnp.concatenate([a_high, a_low], axis=0), b_high, ca, cb)
        return both[rows:] + product(a_high, b_low, ca, cb) + both[:rows]
    return product(a_low, b_high, ca, cb) + product(a_high, b_low, ca, cb) + product(a_high, b_high, ca, cb)


def outer3(a, b):
    a_high, a_low = halves(a)
    b_high, b_low = halves(b)
    return product(
        jnp.concatenate([a_low, a_high, a_high], axis=0),
        jnp.concatenate([b_high, b_low, b_high], axis=0),
        0,
        0,
    )


def iota(shape, dim):
    return lax.broadcasted_iota(jnp.int32, shape, dim)


def far_rows(j, head):
    return pl.ds(TOKENS * j + head % SPACING_WIDE, FAR_ROWS, stride=SPACING_WIDE)


def mid_rows(j, head):
    return pl.ds(TOKENS * j + head % SPACING_CENTRAL, MID_ROWS, stride=SPACING_CENTRAL)


def kernel_call(body, out_shape, operands, scalars, name, scratch=(), from_hbm=()):
    space = pl.BlockSpec(memory_space=pltpu.VMEM)
    in_specs = [pl.BlockSpec(memory_space=pltpu.SMEM)] * scalars + [space] * (
        len(operands) - scalars
    )
    out_specs = jax.tree.map(lambda _: space, out_shape)
    if not INTERPRET:
        operands = [
            pltpu.with_memory_space_constraint(x, pltpu.HBM) if i in from_hbm else x
            for i, x in enumerate(operands)
        ]
    if not INTERPRET and name in TO_HBM:
        out_shape = jax.tree.map(lambda x: pltpu.HBM(x.shape, x.dtype), out_shape)
    return pl.pallas_call(
        body,
        out_shape=out_shape,
        in_specs=in_specs,
        out_specs=out_specs,
        scratch_shapes=[pltpu.VMEM(dims, jnp.float32) for dims in scratch],
        compiler_params=pltpu.CompilerParams(vmem_limit_bytes=16 << 20),
        interpret=INTERPRET,
    )(*operands)


def shaped(*dims):
    return jax.ShapeDtypeStruct(dims, jnp.float32)


def pack_body(count, base, k_ref, v_ref, far_ref, mid_ref, near_ref):
    feature = iota((2 * HEAD, TOKENS), 0)
    live = iota((2 * HEAD, TOKENS), 1) < count[0]
    for j in range(LOCAL_HEADS):
        rows = slice(HEAD * j, HEAD * (j + 1))
        both = jnp.concatenate([k_ref[rows, :], v_ref[rows, :]], axis=0)
        both = jnp.where(live, both, jnp.where(feature == 0, DEAD_MARK, 0.0))
        turned = both.T
        near_ref[TOKENS * j : TOKENS * (j + 1), :] = turned
    for j in range(LOCAL_HEADS):
        head = base[0] + j
        far = near_ref[far_rows(j, head), :]
        mid = near_ref[mid_rows(j, head), :]
        for i in range(far_ref.shape[0]):
            far_ref[i, FAR_ROWS * j : FAR_ROWS * (j + 1), :] = far
        for i in range(mid_ref.shape[0]):
            mid_ref[i, MID_ROWS * j : MID_ROWS * (j + 1), :] = mid


def query_body(count, base, q_ref, w_ref, own_ref, one_ref, two_ref, three_ref, *outs):
    out_ref, cot_ref = outs
    columns = own_ref.shape[0]
    heads = cot_ref.shape[0] // columns
    group = base[0] // LOCAL_HEADS
    for k, ref in enumerate((own_ref, one_ref, two_ref, three_ref)):
        at = pl.multiple_of(columns * ((group + heads - k) % heads), columns)
        cot_ref[pl.ds(at, columns), :] = ref[...]
    live = iota((HEAD, TOKENS), 1) < count[0]
    grads = dot3(w_ref[...], cot_ref[...], 1, 0)
    for j in range(LOCAL_HEADS):
        rows = slice(HEAD * j, HEAD * (j + 1))
        both = jnp.concatenate(
            [q_ref[rows, :] * SCALE, jnp.where(live, grads[rows, :], 0.0)], axis=0
        )
        turned = both.T
        out_ref[head_slice(j, TOKENS), :] = turned
    for j in range(LOCAL_HEADS):
        head = base[0] + j
        far, mid = out_ref[far_rows(j, head), :], out_ref[mid_rows(j, head), :]
        out_ref[NEAR_BLOCK + MID_ROWS * j : NEAR_BLOCK + MID_ROWS * (j + 1), :] = mid
        at = NEAR_BLOCK + MID_BLOCK + FAR_ROWS * j
        out_ref[at : at + FAR_ROWS, :] = far


def split_queries(turned):
    left = iota(turned.shape, 1) < HEAD
    return jnp.concatenate([jnp.where(left, turned, 0.0), jnp.where(left, 0.0, turned)], axis=0)


def branch_scores(turned, pairs):
    rows = turned.shape[0]
    mark = ((iota((16, 2 * HEAD), 0) == 0) & (iota((16, 2 * HEAD), 1) == 0)).astype(jnp.float32)
    products = dot3(jnp.concatenate([split_queries(turned), mark], axis=0), pairs, 1, 1)
    dead = products[2 * rows : 2 * rows + 1, :] > DEAD_LEVEL
    scores = jnp.where(dead, MASKED_SCORE, products[:rows])
    prob_grads = products[rows : 2 * rows]
    top = jnp.max(scores, axis=1, keepdims=True)
    weights = jnp.exp(scores - top)
    total = jnp.sum(weights, axis=1, keepdims=True)
    pulled = jnp.sum(weights * prob_grads, axis=1, keepdims=True)
    at = iota((rows, 128), 1)
    stats = jnp.where(at == 0, top, jnp.where(at == 1, total, pulled))
    return jnp.concatenate([prob_grads, weights], axis=0), stats


def branch_grads(both, factor, delta):
    rows = both.shape[0] // 2
    probs = both[rows:] * factor
    return jnp.concatenate([probs * (both[:rows] - delta), probs], axis=0)


def query_side(both, pairs):
    rows = both.shape[0] // 2
    sums = dot3(both, pairs, 1, 0)
    left = iota((rows, 2 * HEAD), 1) < HEAD
    return jnp.where(left, sums[:rows], sums[rows:])


def gathered(refs, rows):
    parts = []
    for ref in refs:
        part = ref[:, rows, :]
        parts.append(part.reshape(part.shape[0] * part.shape[1], 128))
    return jnp.concatenate(parts, axis=0)


def head_slice(j, rows):
    return slice(rows * j, rows * (j + 1))


def near_pairs_of(own, other, j):
    rows = head_slice(j, TOKENS)
    return jnp.concatenate([own[rows, :], other[rows, :]], axis=0)


def wide_keys(both, turned, refs, j):
    sums = outer3(both, split_queries(turned))
    rows = turned.shape[0]
    half = sums.shape[0] // 2
    for i, ref in enumerate(refs):
        ref[:, head_slice(j, rows), :] = sums[half * i : half * (i + 1)].reshape(
            half // rows, rows, 128
        )


def attention_body(*refs):
    count, base = refs[:2]
    q_ref, near_own, near_other, mid_own, mid_other, cot_ref = refs[2:8]
    far_refs = refs[8:10]
    dq_ref, attended_ref, weight_ref = refs[10:13]
    far_out, mid_out, near_out = refs[13:16]
    far_put, mid_put, back_ref, side_ref = refs[16:]
    each = range(LOCAL_HEADS)
    lanes = iota((TOKENS, 128), 1)
    filler = jnp.where(lanes == 0, MASKED_SCORE, 0.0)
    mid_pairs = [gathered((mid_own, mid_other), head_slice(j, MID_ROWS)) for j in each]
    for j in each:
        far_put[head_slice(j, TOKENS), :] = filler
        mid_put[head_slice(j, TOKENS), :] = filler
    mid_at, far_at = NEAR_BLOCK, NEAR_BLOCK + MID_BLOCK
    near_q = [q_ref[head_slice(j, TOKENS), :] for j in each]
    mid_q = [q_ref[mid_at + MID_ROWS * j : mid_at + MID_ROWS * (j + 1), :] for j in each]
    far_q = [q_ref[far_at + FAR_ROWS * j : far_at + FAR_ROWS * (j + 1), :] for j in each]
    near_pairs = [near_pairs_of(near_own, near_other, j) for j in each]
    far_pairs = [gathered(far_refs, head_slice(j, FAR_ROWS)) for j in each]
    near_starts = [branch_scores(near_q[j], near_pairs[j]) for j in each]
    far_starts = [branch_scores(far_q[j], far_pairs[j]) for j in each]
    starts = [branch_scores(mid_q[j], mid_pairs[j]) for j in each]
    for j in each:
        far_put[far_rows(j, base[0] + j), :] = far_starts[j][1]
        mid_put[mid_rows(j, base[0] + j), :] = starts[j][1]
    factors = []
    far_both, mid_both, near_both = [None] * 3, [None] * 3, [None] * 3
    for j in each:
        far_stats = far_put[head_slice(j, TOKENS), :]
        mid_stats = mid_put[head_slice(j, TOKENS), :]
        near_stats = near_starts[j][1]
        far_top, mid_top, near_top = far_stats[:, 0:1], mid_stats[:, 0:1], near_stats[:, 0:1]
        top = jnp.maximum(near_top, jnp.maximum(mid_top, far_top))
        far_factor = jnp.exp(far_top - top)
        mid_factor = jnp.exp(mid_top - top)
        near_factor = jnp.exp(near_top - top)
        sums = near_factor * near_stats + mid_factor * mid_stats + far_factor * far_stats
        total = sums[:, 1:2]
        delta = sums[:, 2:3] / total
        near_factor = near_factor / total
        back_ref[head_slice(j, TOKENS), :] = jnp.where(
            lanes == 0, far_factor / total, jnp.where(lanes == 1, mid_factor / total, delta)
        )
        factors.append((near_factor, delta))
    for j in each:
        far_back = back_ref[far_rows(j, base[0] + j), :]
        mid_back = back_ref[mid_rows(j, base[0] + j), :]
        near_both[j] = branch_grads(near_starts[j][0], *factors[j])
        mid_both[j] = branch_grads(starts[j][0], mid_back[:, 1:2], mid_back[:, 2:3])
        far_both[j] = branch_grads(far_starts[j][0], far_back[:, 0:1], far_back[:, 2:3])
    for j in each:
        far_out[j] = far_both[j]
        mid_out[j] = mid_both[j]
        near_out[j] = near_both[j]
    for j in each:
        side_ref[head_slice(j, TOKENS), :] = query_side(
            near_both[j], near_pairs[j]
        )
    mid_sides = [query_side(mid_both[j], mid_pairs[j]) for j in each]
    far_sides = [query_side(far_both[j], far_pairs[j]) for j in each]
    for j in each:
        at = mid_rows(j, base[0] + j)
        side_ref[at, :] = side_ref[at, :] + mid_sides[j]
    for j in each:
        at = far_rows(j, base[0] + j)
        side_ref[at, :] = side_ref[at, :] + far_sides[j]
    live = iota((HEAD, TOKENS), 1) < count[0]
    for j in each:
        turned = side_ref[head_slice(j, TOKENS), :].T
        dq_ref[head_slice(j, HEAD), :] = turned[:HEAD] * SCALE
        attended_ref[head_slice(j, HEAD), :] = jnp.where(live, turned[HEAD:], 0.0)
    columns = attended_ref.shape[0]
    weight = dot3(attended_ref[...], cot_ref[...], 1, 1)
    for b in range(weight.shape[1] // 128):
        weight_ref[columns * b : columns * (b + 1), :] = weight[:, 128 * b : 128 * b + 128]


def keys_body(far_both, mid_both, near_both, q_ref, *outs):
    mid_at, far_at = NEAR_BLOCK, NEAR_BLOCK + MID_BLOCK
    for j in range(LOCAL_HEADS):
        mid_q = q_ref[mid_at + MID_ROWS * j : mid_at + MID_ROWS * (j + 1), :]
        far_q = q_ref[far_at + FAR_ROWS * j : far_at + FAR_ROWS * (j + 1), :]
        wide_keys(mid_both[j], mid_q, outs[2:4], j)
        wide_keys(far_both[j], far_q, outs[:2], j)
        sums = dot3(near_both[j], split_queries(q_ref[head_slice(j, TOKENS), :]), 0, 0)
        for i, ref in enumerate(outs[4:]):
            ref[head_slice(j, TOKENS), :] = sums[TOKENS * i : TOKENS * (i + 1)]


def terms_body(base, attended_ref, w_ref, *refs):
    term_refs, terms_ref = refs[:4], refs[4]
    terms_ref[...] = dot3(w_ref[...], attended_ref[...], 0, 0)
    columns = term_refs[0].shape[0]
    heads = terms_ref.shape[0] // columns
    group = base[0] // LOCAL_HEADS
    for k, ref in enumerate(term_refs):
        at = pl.multiple_of(columns * ((group + k) % heads), columns)
        ref[...] = terms_ref[pl.ds(at, columns), :]


def finish_body(base, far_ref, mid_ref, near_ref, other_ref, dk_ref, dv_ref, sum_ref):
    far_sum = far_ref[0, :FAR_BLOCK, :]
    for i in range(1, far_ref.shape[0]):
        far_sum = far_sum + far_ref[i, :FAR_BLOCK, :]
    mid_sum = mid_ref[0, :MID_BLOCK, :]
    for i in range(1, mid_ref.shape[0]):
        mid_sum = mid_sum + mid_ref[i, :MID_BLOCK, :]
    sum_ref[...] = near_ref[...] + other_ref[...]
    for j in range(LOCAL_HEADS):
        at = mid_rows(j, base[0] + j)
        sum_ref[at, :] = sum_ref[at, :] + mid_sum[head_slice(j, MID_ROWS)]
    for j in range(LOCAL_HEADS):
        at = far_rows(j, base[0] + j)
        sum_ref[at, :] = sum_ref[at, :] + far_sum[head_slice(j, FAR_ROWS)]
    for j in range(LOCAL_HEADS):
        turned = sum_ref[head_slice(j, TOKENS), :].T
        dk_ref[head_slice(j, HEAD), :] = turned[:HEAD]
        dv_ref[head_slice(j, HEAD), :] = turned[HEAD:]


def weight_order_body(core, own_ref, other_ref, out_ref, all_ref):
    depth = own_ref.shape[1]
    for i in range(own_ref.shape[0]):
        for ref, c in ((own_ref, core[0]), (other_ref, 1 - core[0])):
            at = pl.multiple_of(depth * (2 * i + c), 8)
            all_ref[pl.ds(at, depth), :] = ref[i]
    rows = out_ref.shape[0]
    for b in range(out_ref.shape[1] // 128):
        out_ref[:, 128 * b : 128 * b + 128] = all_ref[rows * b : rows * (b + 1), :]


def exchange(pieces, axis):
    return lax.all_to_all(pieces, axis, 0, 0, tiled=True)


def to_all(piece, axis):
    return exchange(jnp.broadcast_to(piece, (lax.axis_size(axis), *piece.shape)), axis)


def shifted(x, axis, apart):
    size = lax.axis_size(axis)
    return lax.ppermute(x, axis, [(i, (i + apart) % size) for i in range(size)])


def on_device(queries, keys, values, counts, out_weight, cotangent):
    ny, nz, nzh, nzl = (lax.axis_size(axis) for axis in ("y", Z, "zh", "zl"))
    heads = lax.axis_size("h")
    columns, tokens = queries.shape
    base = (lax.axis_index("h") * LOCAL_HEADS).astype(jnp.int32).reshape(1)

    cots = [cotangent] + [shifted(cotangent, "h", k % heads) for k in range(1, 4)]
    far_out, mid_out, near_own = kernel_call(
        pack_body,
        (shaped(nz, FAR_BLOCK, 128), shaped(nzl, MID_BLOCK, 128), shaped(NEAR_BLOCK, 128)),
        (counts, base, keys, values),
        2,
        "pack",
        (),
        (2, 3),
    )
    near_other = shifted(near_own, "c", 1)
    far_line = exchange(far_out, Z)
    query_rows, full_cot = kernel_call(
        query_body,
        (
            shaped(NEAR_BLOCK + MID_BLOCK + FAR_BLOCK, 128),
            shaped(heads * columns, tokens),
        ),
        (counts, base, queries, out_weight, *cots),
        2,
        "query",
        (),
        (2, 4),
    )
    mid_own = exchange(mid_out, "zl")
    far_lines = [far_line] + [shifted(far_line, "y", k) for k in range(1, ny)]
    far_own = jnp.concatenate(far_lines, axis=0)
    far_other = shifted(far_own, "c", 1)
    mid_other = shifted(mid_own, "c", 1)
    far_keys, mid_keys = 2 * ny * nz * FAR_ROWS, 2 * nzl * MID_ROWS
    query_grad, attended, weight, far_both, mid_both, near_both = kernel_call(
        attention_body,
        (
            shaped(columns, tokens),
            shaped(columns, tokens),
            shaped(out_weight.size // 128, 128),
            shaped(LOCAL_HEADS, 2 * FAR_ROWS, far_keys),
            shaped(LOCAL_HEADS, 2 * MID_ROWS, mid_keys),
            shaped(LOCAL_HEADS, 2 * TOKENS, 2 * TOKENS),
        ),
        (
            counts,
            base,
            query_rows,
            near_own,
            near_other,
            mid_own,
            mid_other,
            full_cot,
            far_own,
            far_other,
        ),
        2,
        "attention",
        ((NEAR_BLOCK, 128),) * 4,
    )
    planes = 2 * ny
    weight_parts = exchange(weight.reshape(planes, -1, 128), ("y", "c"))
    far_keep, far_send, mid_keep, mid_send, near_keep, near_send = kernel_call(
        keys_body,
        (shaped(ny * nz, FAR_BLOCK, 128),) * 2
        + (shaped(nzl, MID_BLOCK, 128),) * 2
        + (shaped(NEAR_BLOCK, 128),) * 2,
        (far_both, mid_both, near_both, query_rows),
        0,
        "keys",
        (),
        (0, 1, 2),
    )
    mid_got = shifted(mid_send, "c", 1)
    weight_line = jnp.sum(weight_parts, axis=0).reshape(nzl, -1, 128)
    mid_total = mid_keep + mid_got
    mid_sums = exchange(jnp.concatenate([mid_total, weight_line], axis=1), "zl")
    far_got = shifted(far_send, "c", 1)
    near_got = shifted(near_send, "c", 1)
    pieces = [far_keep[nz * k : nz * (k + 1)] + far_got[nz * k : nz * (k + 1)] for k in range(ny)]
    pieces = pieces[:1] + [shifted(pieces[k], "y", -k) for k in range(1, ny)]
    far_total = sum(pieces[1:], pieces[0])
    weight_own = jnp.sum(mid_sums[:, MID_BLOCK:], axis=0)
    depth = weight_own.shape[0]
    parts = exchange(
        jnp.concatenate(
            [far_total, jnp.broadcast_to(weight_own, (nz, depth, 128))], axis=1
        ),
        Z,
    )
    terms = kernel_call(
        terms_body,
        (shaped(columns, tokens),) * 4,
        (base, attended, out_weight),
        1,
        "terms",
        ((heads * columns, tokens),),
    )
    got = [terms[0]] + [shifted(terms[k], "h", k % heads) for k in range(1, 4)]
    output = sum(got[1:], got[0])
    weight_whole = jnp.sum(parts[:, FAR_BLOCK:].reshape(nzh, nzl, depth, 128), axis=0)
    own_rows = to_all(weight_whole.reshape(nzl * depth, 128), "y")
    other_rows = shifted(own_rows, "c", 1)
    core = lax.axis_index("c").astype(jnp.int32).reshape(1)
    weight_grad = kernel_call(
        weight_order_body,
        shaped(*out_weight.shape),
        (core, own_rows, other_rows),
        1,
        "weight_order",
        (weight.shape,),
    )
    key_grad, value_grad = kernel_call(
        finish_body,
        (shaped(columns, tokens), shaped(columns, tokens)),
        (base, parts, mid_sums, near_keep, near_got),
        1,
        "finish",
        ((NEAR_BLOCK, 128),),
    )
    return output, query_grad, key_grad, value_grad, weight_grad


def solution(mesh):
    split = Mesh(
        mesh.devices.reshape(4, 2, 8, 2, mesh.shape["head"]), ("y", "zh", "zl", "c", "h")
    )
    return on_mesh(split)


def on_mesh(split):
    in_specs = (
        P("h", SEQ),
        P("h", SEQ),
        P("h", SEQ),
        P(SEQ),
        P("h", None),
        P("h", SEQ),
    )
    out_specs = (P("h", SEQ), P("h", SEQ), P("h", SEQ), P("h", SEQ), P("h", None))
    return jax.shard_map(
        on_device, mesh=split, in_specs=in_specs, out_specs=out_specs, check_vma=False
    )
```
